32 devices in a mesh: rows: 32 (over z, y, x, core).
Axes of the slice: x: 2, y: 2, z: 4, core: 2. Of those that a mesh axis runs over, the one named last changes fastest.
Arguments:
- source: bfloat16 [65536, 128], P('rows'), may hold values from -6 to 6
- target: bfloat16 [65536, 128], P('rows'), may hold values from -6 to 6
- tile_values: bfloat16 [4096, 128, 128], P('rows'), may hold values from -0.25 to 0.25
- tile_rows: int32 [4096], P('rows'), may hold values from 0 to 15
- tile_peers: int32 [4096], P('rows'), may hold values from 0 to 31
- need_list: int32 [32, 32], P('rows'), may hold values from 0 to 15
- tile_count: int32 [32], P('rows'), may hold values from 1 to 128, as said below
Outputs:
- source_embed: bfloat16 [65536, 128], P('rows')
- target_embed: bfloat16 [65536, 128], P('rows')
The draws below stay inside these ranges and needn't reach their ends.
Inputs may be any that keep to these rules, and one draw needn't show every extreme that they name: `tile_count`: some device has 128 live tiles; tiles in slots at or past the count take no part.
All inputs are finite; a program needn't handle non-finite values.
Results may differ from the reference program's by a relative error of at most 0.0053.
Values may be sent and summed in bfloat16 or wider, within the bound.
A program may use at most 128 MiB of HBM per device.

```python
import math
import jax
import jax.numpy as jnp
import numpy as np
from jax import lax

W = 128
BLOCK = 128
RB = 16
TILES_DEV = 128
ITERS = 2
NODES = 65536
DEVICES = 32


def draw_tile_count(key, part):
    ranks = jax.random.permutation(key, DEVICES)
    counts = TILES_DEV * 16 // (16 + ranks)
    return jnp.maximum(counts, 1).astype(jnp.int32)


def plant(values, rng, least, high):
    longest = values.shape.index(max(values.shape))
    spots = []
    for shift in (0, 1):
        where = [jax.random.randint(jax.random.fold_in(rng, axis), (), 0, length) for axis, length in enumerate(values.shape)]
        where[longest] = (where[longest] + shift) % values.shape[longest]
        spots.append(tuple(where))
    return values.at[spots[0]].set(least).at[spots[1]].set(high)


def levels(stream_key, extent, split, smallest, top_value):
    level, own = 1.0, jax.random.fold_in(stream_key, 6)
    for axis_at, shards_of in split:
        draws = jnp.exp(jax.random.uniform(jax.random.fold_in(own, axis_at), (shards_of,), jnp.float32, smallest / len(split), top_value / len(split)))
        level = level * jnp.repeat(draws, extent[axis_at] // shards_of).reshape([-1 if axis == axis_at else 1 for axis in range(len(extent))])
    return level


def cumulative_ranks(amount, skew):
    portions = [(1 << 20) // math.isqrt(grade ** skew) + 1 for grade in range(1, amount + 1)]
    width = 1 + sum(portions) // (1 << 30)
    return np.cumsum(np.array([max(1, weight // width) for weight in portions]))


def ranked(own_key, shape, count, lean):
    grid = cumulative_ranks(count, lean)
    pick = jax.random.randint(jax.random.fold_in(own_key, 1), shape, 0, int(grid[count - 1]))
    grade = jnp.searchsorted(jnp.asarray(grid, jnp.int32), pick, side="right")
    return jax.random.permutation(jax.random.fold_in(own_key, 2), count)[grade].astype(jnp.int32)


def bell_draw(stream_key, shape, deviation, most, cuts=(), kind=jnp.bfloat16):
    values = deviation * jax.random.normal(stream_key, shape, jnp.float32)
    if cuts:
        values = values * levels(stream_key, shape, cuts, -0.22, 0.18)
    return jnp.clip(values, -most, most).astype(kind)


def setup_inputs(seed: int = 0) -> dict:
    arg_keys = jax.random.split(jax.random.key(seed), 8)
    source = bell_draw(arg_keys[0], (NODES, W), 1.0, 6.0, ((0, 32),))
    target = bell_draw(arg_keys[1], (NODES, W), 1.0, 6.0, ((0, 32),))
    tile_values = bell_draw(arg_keys[2], (DEVICES * TILES_DEV, BLOCK, BLOCK), (BLOCK * 4) ** -0.5, 0.25, ((0, 32),))
    tile_rows = plant(jax.random.randint(arg_keys[3], (DEVICES * TILES_DEV,), 0, RB), jax.random.fold_in(arg_keys[3], 1), 0, RB - 1).astype(jnp.int32)
    tile_peers = plant(ranked(arg_keys[4], (DEVICES * TILES_DEV,), DEVICES, 2), jax.random.fold_in(arg_keys[4], 3), 0, DEVICES - 1).astype(jnp.int32)
    need_list = plant(jax.random.randint(arg_keys[5], (DEVICES, DEVICES), 0, RB), jax.random.fold_in(arg_keys[5], 1), 0, RB - 1).astype(jnp.int32)
    tile_count = draw_tile_count(jax.random.fold_in(arg_keys[7], 71), 0)
    return {"source": source, "target": target, "tile_values": tile_values, "tile_rows": tile_rows, "tile_peers": tile_peers, "need_list": need_list, "tile_count": tile_count}


epsilon = 1e-06

def settle(base, update):
    total = base.astype(jnp.float32) + update
    scale = lax.rsqrt(lax.optimization_barrier(jnp.mean(total * total, axis=-1, keepdims=True)) + epsilon)
    return (total * scale).astype(jnp.bfloat16)

def reference(source, target, tile_values, tile_rows, tile_peers, need_list, tile_count):
    tile_side = tile_values.shape[1]
    feature_width = source.shape[1]
    tiles = tile_values.reshape(DEVICES, TILES_DEV, tile_side, tile_side)
    row_ids = tile_rows.reshape(DEVICES, TILES_DEV).astype(jnp.int32)
    peer_ids = tile_peers.reshape(DEVICES, TILES_DEV).astype(jnp.int32)
    device_ids = jnp.arange(DEVICES, dtype=jnp.int32)[:, None]
    row_blocks = device_ids * RB + row_ids
    col_blocks = peer_ids * RB + jnp.take_along_axis(need_list.astype(jnp.int32), peer_ids, axis=1)
    live_mask = (jnp.arange(TILES_DEV, dtype=jnp.int32)[None, :] < tile_count[:, None]).astype(jnp.float32)
    source_now, target_now = (source, target)
    for iteration in range(ITERS):
        source_blocks = source_now.reshape(-1, tile_side, feature_width).astype(jnp.float32)
        target_blocks = target_now.reshape(-1, tile_side, feature_width).astype(jnp.float32)

        def one_device(target_sum, device):
            tile_block = tiles[device].astype(jnp.float32)
            alive = live_mask[device][:, None, None]
            forward = jnp.einsum('tij,tjk->tik', tile_block, source_blocks[col_blocks[device]], precision=lax.Precision.HIGHEST) * alive
            gathered = jax.ops.segment_sum(forward, row_ids[device], num_segments=RB)
            backward = jnp.einsum('tji,tjk->tik', tile_block, target_blocks[row_blocks[device]], precision=lax.Precision.HIGHEST) * alive
            target_sum = target_sum.at[col_blocks[device]].add(backward)
            return (target_sum, gathered)
        start_sum = jnp.zeros((DEVICES * RB, tile_side, feature_width), jnp.float32)
        target_sum, gathered = lax.scan(one_device, start_sum, jnp.arange(DEVICES, dtype=jnp.int32))
        source_now = settle(source, gathered.reshape(-1, feature_width))
        target_now = settle(target, target_sum.reshape(-1, feature_width))
    return (source_now, target_now)
```

```python
import functools

import jax
import jax.numpy as jnp
from jax import lax
from jax.experimental import pallas as pl
from jax.experimental.pallas import tpu as pltpu
from jax.sharding import PartitionSpec as P

ITERS = 2
UNROLL = 4
epsilon = 1e-06
MESH = pl.DeviceIdType.MESH


def lanes_for(count):
    return -(-count // 128) * 128


def index_along(shape, axis):
    return lax.broadcasted_iota(jnp.int32, shape, axis).astype(jnp.float32)


def place_groups(keys, groups, per_slot, slots, out, seat_row, last_row):
    items, lanes = keys.shape[1], lanes_for(groups)
    key = jnp.broadcast_to(keys, (items, items))
    key_down = jnp.broadcast_to(keys, (lanes_for(items), items)).T
    before = (key_down[:, :items] == key) & (
        index_along((items, items), 1) < index_along((items, items), 0)
    )
    rank = jnp.sum(before.astype(jnp.float32), axis=1, keepdims=True)
    lane = index_along((items, lanes), 1)
    member = (jnp.broadcast_to(key_down[:, :1], (items, lanes)) == lane).astype(jnp.float32)
    count = jnp.sum(member, axis=0, keepdims=True)
    used = jnp.floor((count + (per_slot - 1)) * (1.0 / per_slot))
    used_down = jnp.broadcast_to(used, (lanes, lanes)).T
    earlier = (index_along((lanes, lanes), 0) < index_along((lanes, lanes), 1)).astype(jnp.float32)
    start = jnp.sum(used_down * earlier, axis=0, keepdims=True)
    last = jnp.where(used > 0, start + used - 1, float(slots))
    first = jnp.sum(member * start, axis=1, keepdims=True)
    place = jnp.where(key_down[:, :1] >= 0, per_slot * first + rank, -1.0)
    seats = lanes_for(slots * per_slot)
    for chunk in range(seats // 128):
        hot = jnp.broadcast_to(place, (items, 128)) == index_along((items, 128), 1) + 128 * chunk
        item = jnp.where(hot, index_along((items, 128), 0) - items, 0.0)
        chosen = items + jnp.sum(item, axis=0, keepdims=True)
        out[pl.ds(seat_row + chunk, 1), :] = chosen.astype(jnp.int32)
    for chunk in range(lanes // 128):
        out[pl.ds(last_row + chunk, 1), :] = last[:, 128 * chunk : 128 * (chunk + 1)].astype(
            jnp.int32
        )


def slots_for(items, groups):
    pairs = (items + min(items, groups)) // 2
    return -(-pairs // UNROLL) * UNROLL


def kernel(
    n,
    f_slots,
    b_slots,
    row_of,
    peer_of,
    live_count,
    rows_lane,
    peers_lane,
    need,
    source_hbm,
    target_hbm,
    tiles_hbm,
    source_out,
    target_out,
    x_out,
    x_ins,
    y_out,
    y_ins,
    x_now,
    y_now,
    y_base,
    f_sums,
    b_sums,
    c_sums,
    source,
    target,
    tiles,
    need_all,
    need_at,
    tile_plan,
    tile_at,
    part_plan,
    part_at,
    send_sem,
    recv_sem,
    need_send,
    need_recv,
    load_sem,
):
    me = lax.axis_index("rows")
    rows, side, width = source.shape
    tile_total = tiles_hbm.shape[0]
    f_seat, f_last = 0, lanes_for(2 * f_slots) // 128
    b_seat = f_last + lanes_for(rows) // 128
    b_last = b_seat + lanes_for(2 * b_slots) // 128
    c_last = lanes_for(n) // 128

    barrier = pltpu.get_barrier_semaphore()

    def greet(k, carry):
        pl.semaphore_signal(
            barrier, inc=1, device_id=(lax.rem(me + k, n),), device_id_type=MESH
        )
        return carry

    lax.fori_loop(1, n, greet, 0)
    source_load = pltpu.make_async_copy(source_hbm, source, load_sem.at[5])
    source_load.start()
    target_load = pltpu.make_async_copy(target_hbm, target, load_sem.at[0])
    target_load.start()
    tile_load = pltpu.make_async_copy(tiles_hbm, tiles.at[pl.ds(0, tile_total)], load_sem.at[1])
    tile_load.start()

    zero_block = jnp.zeros((side, width), jnp.bfloat16)
    zero_sum = jnp.zeros((side, width), jnp.float32)
    tiles[tile_total] = jnp.zeros((side, side), jnp.bfloat16)
    f_sums[f_slots] = zero_sum
    b_sums[b_slots] = zero_block
    c_sums[n] = zero_sum
    need_all[me] = need[...]
    pl.semaphore_wait(barrier, n - 1)

    def ask(k, carry):
        pltpu.make_async_remote_copy(
            src_ref=need,
            dst_ref=need_all.at[me],
            send_sem=need_send.at[0],
            recv_sem=need_recv.at[0],
            device_id=(lax.rem(me + k, n),),
            device_id_type=MESH,
        ).start()
        return carry

    lax.fori_loop(1, n, ask, 0)

    def turn(b, carry):
        flipped = target[b].astype(jnp.float32).T
        y_base[b] = flipped
        y_now[b] = flipped.astype(jnp.bfloat16)
        return carry

    def plan_tiles():
        live = lax.broadcasted_iota(jnp.int32, (1, tile_total), 1) < live_count[0]
        row_keys = jnp.where(live, rows_lane[...], -1).astype(jnp.float32)
        peer_keys = jnp.where(live, peers_lane[...], -1).astype(jnp.float32)
        place_groups(row_keys, rows, 2, f_slots, tile_plan, f_seat, f_last)
        place_groups(peer_keys, n, 2, b_slots, tile_plan, b_seat, b_last)
        load = pltpu.make_async_copy(tile_plan, tile_at, load_sem.at[3])
        load.start()
        load.wait()

    def plan_parts():
        table = need_all[...].reshape(n, need_all.shape[2]).astype(jnp.float32)
        mine = index_along(table.shape, 1) == me.astype(jnp.float32)
        wanted = jnp.sum(jnp.where(mine, table, 0.0), axis=1, keepdims=True)
        keys = jnp.broadcast_to(wanted, (n, 128)).T[:1]
        place_groups(keys, rows, 1, n, part_plan, 0, c_last)
        load = pltpu.make_async_copy(part_plan, part_at, load_sem.at[4])
        load.start()
        load.wait()

    def seat(table, first, index, top):
        return jnp.clip(table[first + index // 128, index % 128], 0, top)

    def tile_pair(first, q):
        left = seat(tile_at, first, 2 * q, tile_total)
        right = seat(tile_at, first, 2 * q + 1, tile_total)
        return left, right, jnp.minimum(left, tile_total - 1), jnp.minimum(right, tile_total - 1)

    def asked(d):
        return jnp.clip(need_at[d, 0, me], 0, rows - 1)

    def send(out, inn, phase, it, fill):
        def one(k, carry):
            peer = lax.rem(me + k, n)
            out[it, peer] = fill(peer)
            pltpu.make_async_remote_copy(
                src_ref=out.at[it, peer],
                dst_ref=inn.at[me],
                send_sem=send_sem.at[phase],
                recv_sem=recv_sem.at[phase],
                device_id=(peer,),
                device_id_type=MESH,
            ).start()
            return carry

        lax.fori_loop(1, n, one, 0)
        inn[me] = fill(me)

    def all_of(buffer, sem):
        view = buffer.at[pl.ds(0, n - 1)]
        pltpu.make_async_copy(view, view, sem).wait()

    def send_x(blocks, it):
        send(x_out, x_ins[it], 2 * it, it, lambda p: blocks[asked(p)])

    def backward(it):
        def one(q, carry):
            total, key = carry
            left, right, left_at, right_at = tile_pair(b_seat, q)
            flipped = jnp.concatenate([y_now[row_of[left_at]], y_now[row_of[right_at]]], axis=1)
            stack = jnp.concatenate([tiles[left], tiles[right]], axis=0)
            product = jnp.dot(flipped, stack, preferred_element_type=jnp.float32)
            new_key = peer_of[left_at]
            total = total * (new_key == key).astype(jnp.float32) + product
            b_sums[q] = total.astype(jnp.bfloat16)
            return total, new_key

        lax.fori_loop(0, b_slots, one, (zero_sum, jnp.int32(-1)), unroll=UNROLL)
        send(y_out, y_ins[it], 2 * it + 1, it, lambda p: b_sums[seat(tile_at, b_last, p, b_slots)])

    def forward(it, result):
        x_in = x_ins[it]
        all_of(x_in, recv_sem.at[2 * it])

        def one(q, carry):
            total, key = carry
            left, right, left_at, right_at = tile_pair(f_seat, q)
            stack = jnp.concatenate([tiles[left], tiles[right]], axis=1)
            blocks = jnp.concatenate([x_in[peer_of[left_at]], x_in[peer_of[right_at]]], axis=0)
            product = jnp.dot(stack, blocks, preferred_element_type=jnp.float32)
            new_key = row_of[left_at]
            total = total * (new_key == key).astype(jnp.float32) + product
            f_sums[q] = total
            return total, new_key

        lax.fori_loop(0, f_slots, one, (zero_sum, jnp.int32(-1)), unroll=UNROLL)

        def settle(b, carry):
            total = source[b].astype(jnp.float32) + f_sums[seat(tile_at, f_last, b, f_slots)]
            scale = lax.rsqrt(jnp.mean(total * total, axis=-1, keepdims=True) + epsilon)
            result[b] = (total * scale).astype(jnp.bfloat16)
            return carry

        lax.fori_loop(0, rows, settle, 0)

    def combine(it, final):
        y_in = y_ins[it]
        all_of(y_in, recv_sem.at[2 * it + 1])

        def one(k, carry):
            total, key = carry
            sender = seat(part_at, 0, k, n - 1)
            new_key = asked(sender)
            total = total * (new_key == key).astype(jnp.float32) + y_in[sender].astype(jnp.float32)
            c_sums[k] = total
            return total, new_key

        lax.fori_loop(0, n, one, (zero_sum, jnp.int32(-1)), unroll=UNROLL)

        def settle(b, carry):
            total = y_base[b] + c_sums[seat(part_at, c_last, b, n)]
            scale = lax.rsqrt(jnp.mean(total * total, axis=0, keepdims=True) + epsilon)
            if final:
                target_out[b] = (total * scale).T.astype(jnp.bfloat16)
            else:
                y_now[b] = (total * scale).astype(jnp.bfloat16)
            return carry

        lax.fori_loop(0, rows, settle, 0)

    all_of(need_all, need_recv.at[0])
    need_load = pltpu.make_async_copy(need_all, need_at, load_sem.at[2])
    need_load.start()
    need_load.wait()
    source_load.wait()
    send_x(source, 0)
    plan_tiles()
    target_load.wait()
    lax.fori_loop(0, rows, turn, 0)
    tile_load.wait()
    backward(0)
    plan_parts()
    for it in range(ITERS):
        final = it == ITERS - 1
        forward(it, source_out if final else x_now)
        if not final:
            send_x(x_now, it + 1)
        combine(it, final)
        if not final:
            backward(it + 1)
    all_of(need_all, need_send.at[0])
    for it in range(ITERS):
        all_of(x_out.at[it], send_sem.at[2 * it])
        all_of(y_out.at[it], send_sem.at[2 * it + 1])


def shards(source, target, tile_values, tile_rows, tile_peers, need_list, tile_count):
    n = lax.axis_size("rows")
    tiles_here, side, _ = tile_values.shape
    width = source.shape[1]
    rows = source.shape[0] // side
    f_slots = slots_for(tiles_here, rows)
    b_slots = slots_for(tiles_here, n)
    tile_plan = (
        lanes_for(2 * f_slots) + lanes_for(rows) + lanes_for(2 * b_slots) + lanes_for(n)
    ) // 128
    part_plan = (lanes_for(n) + lanes_for(rows)) // 128
    block = (side, width)
    vmem = pl.BlockSpec(memory_space=pltpu.VMEM)
    smem = pl.BlockSpec(memory_space=pltpu.SMEM)
    source_now, target_now = pl.pallas_call(
        functools.partial(kernel, n, f_slots, b_slots),
        out_shape=[pltpu.VMEM((rows,) + block, jnp.bfloat16)] * 2,
        in_specs=[smem] * 3 + [vmem] * 3 + [pl.BlockSpec(memory_space=pltpu.HBM)] * 3,
        out_specs=[vmem, vmem],
        scratch_shapes=[
            pltpu.VMEM((ITERS, n) + block, jnp.bfloat16),
            [pltpu.VMEM((n,) + block, jnp.bfloat16)] * ITERS,
            pltpu.VMEM((ITERS, n) + block, jnp.bfloat16),
            [pltpu.VMEM((n,) + block, jnp.bfloat16)] * ITERS,
            pltpu.VMEM((rows,) + block, jnp.bfloat16),
            pltpu.VMEM((rows,) + block, jnp.bfloat16),
            pltpu.VMEM((rows,) + block, jnp.float32),
            pltpu.VMEM((f_slots + 1,) + block, jnp.float32),
            pltpu.VMEM((b_slots + 1,) + block, jnp.bfloat16),
            pltpu.VMEM((n + 1,) + block, jnp.float32),
            pltpu.VMEM((rows,) + block, jnp.bfloat16),
            pltpu.VMEM((rows,) + block, jnp.bfloat16),
            pltpu.VMEM((tiles_here + 1, side, side), jnp.bfloat16),
            pltpu.VMEM((n, 1, n), jnp.int32),
            pltpu.SMEM((n, 1, n), jnp.int32),
            pltpu.VMEM((tile_plan, 128), jnp.int32),
            pltpu.SMEM((tile_plan, 128), jnp.int32),
            pltpu.VMEM((part_plan, 128), jnp.int32),
            pltpu.SMEM((part_plan, 128), jnp.int32),
            pltpu.SemaphoreType.DMA((2 * ITERS,)),
            pltpu.SemaphoreType.DMA((2 * ITERS,)),
            pltpu.SemaphoreType.DMA((1,)),
            pltpu.SemaphoreType.DMA((1,)),
            pltpu.SemaphoreType.DMA((6,)),
        ],
        compiler_params=pltpu.CompilerParams(
            collective_id=0, has_side_effects=True, vmem_limit_bytes=60000000
        ),
    )(
        tile_rows,
        tile_peers,
        tile_count,
        tile_rows.reshape(1, -1),
        tile_peers.reshape(1, -1),
        need_list,
        source.reshape((rows,) + block),
        target.reshape((rows,) + block),
        tile_values,
    )
    return source_now.reshape(-1, width), target_now.reshape(-1, width)


def solution(mesh):
    return jax.shard_map(
        shards,
        mesh=mesh,
        in_specs=(
            P("rows", None),
            P("rows", None),
            P("rows", None, None),
            P("rows"),
            P("rows"),
            P("rows", None),
            P("rows"),
        ),
        out_specs=(P("rows", None), P("rows", None)),
        check_vma=False,
    )
```

```python
import functools

import jax
import jax.numpy as jnp
from jax import lax
from jax.experimental import pallas as pl
from jax.experimental.pallas import tpu as pltpu
from jax.sharding import PartitionSpec as P

ITERS = 2
UNROLL = 4
epsilon = 1e-06
MESH = pl.DeviceIdType.MESH


def lanes_for(count):
    return -(-count // 128) * 128


def index_along(shape, axis):
    return lax.broadcasted_iota(jnp.int32, shape, axis).astype(jnp.float32)


def place_groups(keys, groups, per_slot, slots, out, seat_row, last_row):
    items, lanes = keys.shape[1], lanes_for(groups)
    key = jnp.broadcast_to(keys, (items, items))
    key_down = jnp.broadcast_to(keys, (lanes_for(items), items)).T
    before = (key_down[:, :items] == key) & (
        index_along((items, items), 1) < index_along((items, items), 0)
    )
    rank = jnp.sum(before.astype(jnp.float32), axis=1, keepdims=True)
    lane = index_along((items, lanes), 1)
    member = (jnp.broadcast_to(key_down[:, :1], (items, lanes)) == lane).astype(jnp.float32)
    count = jnp.sum(member, axis=0, keepdims=True)
    used = jnp.floor((count + (per_slot - 1)) * (1.0 / per_slot))
    used_down = jnp.broadcast_to(used, (lanes, lanes)).T
    earlier = (index_along((lanes, lanes), 0) < index_along((lanes, lanes), 1)).astype(jnp.float32)
    start = jnp.sum(used_down * earlier, axis=0, keepdims=True)
    last = jnp.where(used > 0, start + used - 1, float(slots))
    first = jnp.sum(member * start, axis=1, keepdims=True)
    place = jnp.where(key_down[:, :1] >= 0, per_slot * first + rank, -1.0)
    seats = lanes_for(slots * per_slot)
    for chunk in range(seats // 128):
        hot = jnp.broadcast_to(place, (items, 128)) == index_along((items, 128), 1) + 128 * chunk
        item = jnp.where(hot, index_along((items, 128), 0) - items, 0.0)
        chosen = items + jnp.sum(item, axis=0, keepdims=True)
        out[pl.ds(seat_row + chunk, 1), :] = chosen.astype(jnp.int32)
    for chunk in range(lanes // 128):
        out[pl.ds(last_row + chunk, 1), :] = last[:, 128 * chunk : 128 * (chunk + 1)].astype(
            jnp.int32
        )


def slots_for(items, groups):
    pairs = (items + min(items, groups)) // 2
    return -(-pairs // UNROLL) * UNROLL


def read_peers(peer_keys, lanes):
    items = peer_keys.shape[1]
    key_down = jnp.broadcast_to(peer_keys, (lanes_for(items), items)).T
    member = jnp.broadcast_to(key_down[:, :1], (items, lanes)) == index_along((items, lanes), 1)
    return jnp.sum(member.astype(jnp.float32), axis=0, keepdims=True)


def general(
    n,
    f_slots,
    b_slots,
    row_of,
    peer_of,
    live_count,
    rows_lane,
    peers_lane,
    need,
    source_hbm,
    target_hbm,
    tiles_hbm,
    source_out,
    target_out,
    x_out,
    x_ins,
    y_out,
    y_ins,
    x_now,
    y_now,
    y_base,
    f_sums,
    b_sums,
    c_sums,
    source,
    target,
    tiles,
    need_all,
    need_at,
    tile_plan,
    tile_at,
    part_plan,
    part_at,
    send_sem,
    recv_sem,
    need_send,
    need_recv,
    load_sem,
):
    me = lax.axis_index("rows")
    rows, side, width = source.shape
    tile_total = tiles_hbm.shape[0]
    f_seat, f_last = 0, lanes_for(2 * f_slots) // 128
    b_seat = f_last + lanes_for(rows) // 128
    b_last = b_seat + lanes_for(2 * b_slots) // 128
    c_last = lanes_for(n) // 128

    barrier = pltpu.get_barrier_semaphore()

    def greet(k, carry):
        pl.semaphore_signal(
            barrier, inc=1, device_id=(lax.rem(me + k, n),), device_id_type=MESH
        )
        return carry

    lax.fori_loop(1, n, greet, 0)
    source_load = pltpu.make_async_copy(source_hbm, source, load_sem.at[5])
    source_load.start()
    target_load = pltpu.make_async_copy(target_hbm, target, load_sem.at[0])
    target_load.start()
    tile_load = pltpu.make_async_copy(tiles_hbm, tiles.at[pl.ds(0, tile_total)], load_sem.at[1])
    tile_load.start()

    zero_block = jnp.zeros((side, width), jnp.bfloat16)
    zero_sum = jnp.zeros((side, width), jnp.float32)
    tiles[tile_total] = jnp.zeros((side, side), jnp.bfloat16)
    f_sums[f_slots] = zero_sum
    b_sums[b_slots] = zero_block
    c_sums[n] = zero_sum
    need_all[me] = need[...]
    pl.semaphore_wait(barrier, n - 1)

    def ask(k, carry):
        pltpu.make_async_remote_copy(
            src_ref=need,
            dst_ref=need_all.at[me],
            send_sem=need_send.at[0],
            recv_sem=need_recv.at[0],
            device_id=(lax.rem(me + k, n),),
            device_id_type=MESH,
        ).start()
        return carry

    lax.fori_loop(1, n, ask, 0)

    def turn(b, carry):
        flipped = target[b].astype(jnp.float32).T
        y_base[b] = flipped
        y_now[b] = flipped.astype(jnp.bfloat16)
        return carry

    def plan_tiles():
        live = lax.broadcasted_iota(jnp.int32, (1, tile_total), 1) < live_count[0]
        row_keys = jnp.where(live, rows_lane[...], -1).astype(jnp.float32)
        peer_keys = jnp.where(live, peers_lane[...], -1).astype(jnp.float32)
        place_groups(row_keys, rows, 2, f_slots, tile_plan, f_seat, f_last)
        place_groups(peer_keys, n, 2, b_slots, tile_plan, b_seat, b_last)
        load = pltpu.make_async_copy(tile_plan, tile_at, load_sem.at[3])
        load.start()
        load.wait()

    def plan_parts():
        table = need_all[...].reshape(n, need_all.shape[2]).astype(jnp.float32)
        mine = index_along(table.shape, 1) == me.astype(jnp.float32)
        wanted = jnp.sum(jnp.where(mine, table, 0.0), axis=1, keepdims=True)
        keys = jnp.broadcast_to(wanted, (n, 128)).T[:1]
        place_groups(keys, rows, 1, n, part_plan, 0, c_last)
        load = pltpu.make_async_copy(part_plan, part_at, load_sem.at[4])
        load.start()
        load.wait()

    def seat(table, first, index, top):
        return jnp.clip(table[first + index // 128, index % 128], 0, top)

    def tile_pair(first, q):
        left = seat(tile_at, first, 2 * q, tile_total)
        right = seat(tile_at, first, 2 * q + 1, tile_total)
        return left, right, jnp.minimum(left, tile_total - 1), jnp.minimum(right, tile_total - 1)

    def asked(d):
        return jnp.clip(need_at[d, 0, me], 0, rows - 1)

    def send(out, inn, phase, it, fill):
        def one(k, carry):
            peer = lax.rem(me + k, n)
            out[it, peer] = fill(peer)
            pltpu.make_async_remote_copy(
                src_ref=out.at[it, peer],
                dst_ref=inn.at[me],
                send_sem=send_sem.at[phase],
                recv_sem=recv_sem.at[phase],
                device_id=(peer,),
                device_id_type=MESH,
            ).start()
            return carry

        lax.fori_loop(1, n, one, 0)
        inn[me] = fill(me)

    def all_of(buffer, sem):
        view = buffer.at[pl.ds(0, n - 1)]
        pltpu.make_async_copy(view, view, sem).wait()

    def send_x(blocks, it):
        send(x_out, x_ins[it], 2 * it, it, lambda p: blocks[asked(p)])

    def backward(it):
        def one(q, carry):
            total, key = carry
            left, right, left_at, right_at = tile_pair(b_seat, q)
            flipped = jnp.concatenate([y_now[row_of[left_at]], y_now[row_of[right_at]]], axis=1)
            stack = jnp.concatenate([tiles[left], tiles[right]], axis=0)
            product = jnp.dot(flipped, stack, preferred_element_type=jnp.float32)
            new_key = peer_of[left_at]
            total = total * (new_key == key).astype(jnp.float32) + product
            b_sums[q] = total.astype(jnp.bfloat16)
            return total, new_key

        lax.fori_loop(0, b_slots, one, (zero_sum, jnp.int32(-1)), unroll=UNROLL)
        send(y_out, y_ins[it], 2 * it + 1, it, lambda p: b_sums[seat(tile_at, b_last, p, b_slots)])

    def forward(it, result):
        x_in = x_ins[it]
        all_of(x_in, recv_sem.at[2 * it])

        def one(q, carry):
            total, key = carry
            left, right, left_at, right_at = tile_pair(f_seat, q)
            stack = jnp.concatenate([tiles[left], tiles[right]], axis=1)
            blocks = jnp.concatenate([x_in[peer_of[left_at]], x_in[peer_of[right_at]]], axis=0)
            product = jnp.dot(stack, blocks, preferred_element_type=jnp.float32)
            new_key = row_of[left_at]
            total = total * (new_key == key).astype(jnp.float32) + product
            f_sums[q] = total
            return total, new_key

        lax.fori_loop(0, f_slots, one, (zero_sum, jnp.int32(-1)), unroll=UNROLL)

        def settle(b, carry):
            total = source[b].astype(jnp.float32) + f_sums[seat(tile_at, f_last, b, f_slots)]
            scale = lax.rsqrt(jnp.mean(total * total, axis=-1, keepdims=True) + epsilon)
            result[b] = (total * scale).astype(jnp.bfloat16)
            return carry

        lax.fori_loop(0, rows, settle, 0)

    def combine(it, final):
        y_in = y_ins[it]
        all_of(y_in, recv_sem.at[2 * it + 1])

        def one(k, carry):
            total, key = carry
            sender = seat(part_at, 0, k, n - 1)
            new_key = asked(sender)
            total = total * (new_key == key).astype(jnp.float32) + y_in[sender].astype(jnp.float32)
            c_sums[k] = total
            return total, new_key

        lax.fori_loop(0, n, one, (zero_sum, jnp.int32(-1)), unroll=UNROLL)

        def settle(b, carry):
            total = y_base[b] + c_sums[seat(part_at, c_last, b, n)]
            scale = lax.rsqrt(jnp.mean(total * total, axis=0, keepdims=True) + epsilon)
            if final:
                target_out[b] = (total * scale).T.astype(jnp.bfloat16)
            else:
                y_now[b] = (total * scale).astype(jnp.bfloat16)
            return carry

        lax.fori_loop(0, rows, settle, 0)

    all_of(need_all, need_recv.at[0])
    need_load = pltpu.make_async_copy(need_all, need_at, load_sem.at[2])
    need_load.start()
    need_load.wait()
    source_load.wait()
    send_x(source, 0)
    plan_tiles()
    target_load.wait()
    lax.fori_loop(0, rows, turn, 0)
    tile_load.wait()
    backward(0)
    plan_parts()
    for it in range(ITERS):
        final = it == ITERS - 1
        forward(it, source_out if final else x_now)
        if not final:
            send_x(x_now, it + 1)
        combine(it, final)
        if not final:
            backward(it + 1)
    all_of(need_all, need_send.at[0])
    for it in range(ITERS):
        all_of(x_out.at[it], send_sem.at[2 * it])
        all_of(y_out.at[it], send_sem.at[2 * it + 1])


def fast(
    n,
    cap,
    f_slots,
    b_slots,
    row_of,
    peer_of,
    live_count,
    rows_lane,
    peers_lane,
    need,
    source_hbm,
    target_hbm,
    tiles_hbm,
    source_out,
    target_out,
    over_out,
    x_near_out,
    x_far_out,
    x_ins,
    gates,
    relay_out,
    y_out,
    y_near_ins,
    y_gates,
    y_cross_out,
    y_far_ins,
    x_now,
    y_now,
    y_base,
    y_mid,
    f_sums,
    b_sums,
    c_sums,
    source,
    target,
    tiles,
    need_mine,
    need_all,
    need_at,
    tile_plan,
    tile_at,
    part_plan,
    part_at,
    far_plan,
    far_at,
    x_send,
    x_recv,
    gate_send,
    gate_recv,
    relay_send,
    y_send,
    y_near_recv,
    y_gate_recv,
    y_cross_send,
    y_far_recv,
    need_send,
    need_recv,
    load_sem,
):
    me = lax.axis_index("rows")
    rows, side, width = source.shape
    tile_total = tiles_hbm.shape[0]
    lanes = lanes_for(n)
    half, plane = n // 2, n // 4
    upper = me // half
    near_first, far_first = upper * half, (1 - upper) * half
    spot, column = me % half, me % plane
    inner = me // plane == 1 + upper
    outer = jnp.logical_not(inner)
    far_gate = (2 - upper) * plane + column
    near_gates = (1 + upper) * plane
    far_planes = (3 * (1 - upper) * plane, (2 - upper) * plane)
    far_owner = tuple(first + column for first in far_planes)
    f_seat, f_last = 0, lanes_for(2 * f_slots) // 128
    b_seat = f_last + lanes_for(rows) // 128
    b_last = b_seat + lanes_for(2 * b_slots) // 128
    c_last = lanes_for(n) // 128
    part_rows = c_last + lanes_for(rows) // 128
    far_list = n
    far_slot = n + rows

    barrier = pltpu.get_barrier_semaphore()

    def greet(k, carry):
        pl.semaphore_signal(
            barrier, inc=1, device_id=(lax.rem(me + k, n),), device_id_type=MESH
        )
        return carry

    lax.fori_loop(1, n, greet, 0)
    source_load = pltpu.make_async_copy(source_hbm, source, load_sem.at[5])
    source_load.start()
    target_load = pltpu.make_async_copy(target_hbm, target, load_sem.at[0])
    target_load.start()
    tile_load = pltpu.make_async_copy(tiles_hbm, tiles.at[pl.ds(0, tile_total)], load_sem.at[1])
    tile_load.start()

    live = lax.broadcasted_iota(jnp.int32, (1, tile_total), 1) < live_count[0]
    row_keys = jnp.where(live, rows_lane[...], -1).astype(jnp.float32)
    peer_keys = jnp.where(live, peers_lane[...], -1).astype(jnp.float32)
    read = read_peers(peer_keys, lanes)
    need_mine[...] = jnp.full((1, lanes), -1, jnp.int32)
    need_mine[:, :n] = jnp.where(read[:, :n] > 0, need[...], -1)
    zero_block = jnp.zeros((side, width), jnp.bfloat16)
    zero_sum = jnp.zeros((side, width), jnp.float32)
    tiles[tile_total] = jnp.zeros((side, side), jnp.bfloat16)
    f_sums[f_slots] = zero_sum
    b_sums[b_slots] = zero_block
    c_sums[half] = zero_sum
    for it in range(ITERS):
        y_far_ins[it][cap] = zero_block
    need_all[me] = need_mine[...]
    def turn(b, carry):
        flipped = target[b].astype(jnp.float32).T
        y_base[b] = flipped
        y_now[b] = flipped.astype(jnp.bfloat16)
        return carry

    def plan_tiles():
        place_groups(row_keys, rows, 2, f_slots, tile_plan, f_seat, f_last)
        place_groups(peer_keys, n, 2, b_slots, tile_plan, b_seat, b_last)
        load = pltpu.make_async_copy(tile_plan, tile_at, load_sem.at[3])
        load.start()
        load.wait()

    plan_tiles()
    target_load.wait()
    lax.fori_loop(0, rows, turn, 0)
    source_load.wait()
    pl.semaphore_wait(barrier, n - 1)

    def push(src, dst, send_sem, recv_sem, peer):
        pltpu.make_async_remote_copy(
            src_ref=src,
            dst_ref=dst,
            send_sem=send_sem,
            recv_sem=recv_sem,
            device_id=(peer,),
            device_id_type=MESH,
        ).start()

    def all_of(buffer, count, sem):
        view = buffer.at[pl.ds(0, count)]
        pltpu.make_async_copy(view, view, sem).wait()

    def ask(k, carry):
        peer = lax.rem(me + k, n)
        push(need_mine, need_all.at[me], need_send.at[0], need_recv.at[0], peer)
        return carry

    lax.fori_loop(1, n, ask, 0)

    def send_whole(s, first, count):
        push(
            source.at[pl.ds(first, count)],
            gates[0][s].at[pl.ds(first, count)],
            gate_send.at[0],
            gate_recv.at[s],
            far_gate,
        )

    def needs():
        return need_all[...].reshape(n, lanes).astype(jnp.float32)

    def plan_far():
        table = needs()
        early = index_along((1, lanes), 1) < half
        before = jnp.zeros((1, lanes), jnp.float32)
        place = jnp.zeros((n, lanes), jnp.float32)
        listed = jnp.zeros((rows, lanes), jnp.float32)
        for b in range(rows):
            hit = (table == b).astype(jnp.float32)
            low = jnp.max(hit[:half], axis=0, keepdims=True)
            high = jnp.max(hit[half:], axis=0, keepdims=True)
            used = jnp.where(early, high, low)
            place = place + hit * before
            chosen = jnp.where(used > 0, before, -1.0)
            listed = jnp.where(index_along((rows, lanes), 0) == chosen, float(b), listed)
            far_plan[pl.ds(far_slot + b, 1), :] = jnp.where(used > 0, before, float(cap)).astype(
                jnp.int32
            )
            before = before + used
        far_plan[pl.ds(0, n), :] = place.astype(jnp.int32)
        far_plan[pl.ds(far_list, rows), :] = listed.astype(jnp.int32)
        worst = jnp.max(before, axis=1, keepdims=True)
        over_out[...] = (worst > cap).astype(jnp.int32)
        load = pltpu.make_async_copy(far_plan, far_at, load_sem.at[6])
        load.start()
        load.wait()

    def plan_parts():
        table = needs()
        sender = index_along((n, lanes), 0)
        lane = index_along((n, lanes), 1)
        near = (sender >= near_first.astype(jnp.float32)) & (
            sender < (near_first + half).astype(jnp.float32)
        )
        known = near & (table >= 0)
        place = far_plan[pl.ds(0, n), :].astype(jnp.float32)

        def column_of(values, at):
            mine = lane == at.astype(jnp.float32)
            column = jnp.sum(jnp.where(mine, values, 0.0), axis=1, keepdims=True)
            return jnp.broadcast_to(column, (n, 128)).T[:1]

        def plan(values, at, first):
            keys = column_of(jnp.where(known, values, -1.0), at)
            place_groups(keys, rows, 1, half, part_plan, first, first + c_last)

        plan(table, me, 0)
        for s in range(2):
            plan(place, far_owner[s], (1 + s) * part_rows)
        load = pltpu.make_async_copy(part_plan, part_at, load_sem.at[4])
        load.start()
        load.wait()

    def seat(table, first, index, top):
        return jnp.clip(table[first + index // 128, index % 128], 0, top)

    def tile_pair(first, q):
        left = seat(tile_at, first, 2 * q, tile_total)
        right = seat(tile_at, first, 2 * q + 1, tile_total)
        return left, right, jnp.minimum(left, tile_total - 1), jnp.minimum(right, tile_total - 1)

    def asked(d):
        return jnp.clip(need_at[d, 0, me], 0, rows - 1)

    def send_near(blocks, it):
        x_in = x_ins[it]
        if it:
            all_of(x_in, half - 1, x_send.at[it - 1])

        def one(k, carry):
            peer = near_first + lax.rem(spot + k, half)
            x_near_out[k] = blocks[asked(peer)]
            push(x_near_out.at[k], x_in.at[me], x_send.at[it], x_recv.at[it], peer)
            return carry

        lax.fori_loop(1, half, one, 0)
        x_in[me] = blocks[asked(me)]

    def send_far(blocks, it, s):
        def one(i, carry):
            x_far_out[i] = blocks[jnp.clip(far_at[far_list + i, me], 0, rows - 1)]
            return carry

        lax.fori_loop(0, cap, one, 0)
        push(
            x_far_out,
            gates[it][s].at[pl.ds(0, cap)],
            gate_send.at[it],
            gate_recv.at[2 * it + s],
            far_gate,
        )

    def relay(it, s, whole):
        gate, x_in, owner = gates[it][s], x_ins[it], far_owner[s]
        if it:
            all_of(x_in, half - 1, relay_send.at[2 * (it - 1) + s])
        all_of(gate, rows if whole else cap, gate_recv.at[2 * it + s])

        def block(d):
            at = need_at[d, 0, owner] if whole else far_at[d, owner]
            return gate[jnp.clip(at, 0, (rows if whole else cap) - 1)]

        def one(k, carry):
            peer = near_first + lax.rem(spot + k, half)
            relay_out[s, k] = block(peer)
            push(
                relay_out.at[s, k],
                x_in.at[owner],
                relay_send.at[2 * it + s],
                x_recv.at[it],
                peer,
            )
            return carry

        lax.fori_loop(1, half, one, 0)
        x_in[owner] = block(me)

    def backward(it):
        def one(q, carry):
            total, key = carry
            left, right, left_at, right_at = tile_pair(b_seat, q)
            flipped = jnp.concatenate([y_now[row_of[left_at]], y_now[row_of[right_at]]], axis=1)
            stack = jnp.concatenate([tiles[left], tiles[right]], axis=0)
            product = jnp.dot(flipped, stack, preferred_element_type=jnp.float32)
            new_key = peer_of[left_at]
            total = total * (new_key == key).astype(jnp.float32) + product
            b_sums[q] = total.astype(jnp.bfloat16)
            return total, new_key

        lax.fori_loop(0, b_slots, one, (zero_sum, jnp.int32(-1)), unroll=UNROLL)

    def part(peer):
        return b_sums[seat(tile_at, b_last, peer, b_slots)]

    def send_parts(it, s):
        gate_in = y_gates[it][s]

        def one(k, carry):
            gate = lax.rem(column + k, plane)
            peer = far_planes[s] + gate
            y_out[peer] = part(peer)
            push(
                y_out.at[peer],
                gate_in.at[spot],
                y_send.at[it],
                y_gate_recv.at[2 * it + s],
                near_gates + gate,
            )
            return carry

        @pl.when(outer)
        def _():
            one(0, 0)

        @pl.when(inner)
        def _():
            gate_in[spot] = part(far_owner[s])

        lax.fori_loop(1, plane, one, 0)

    def send_near_parts(it):
        def one(k, carry):
            peer = near_first + lax.rem(spot + k, half)
            y_out[peer] = part(peer)
            push(y_out.at[peer], y_near_ins[it].at[spot], y_send.at[it], y_near_recv.at[it], peer)
            return carry

        lax.fori_loop(1, half, one, 0)
        y_near_ins[it][spot] = part(me)

    def sent_parts(it):
        @pl.when(inner)
        def _():
            all_of(y_out, n - 3, y_send.at[it])

        @pl.when(outer)
        def _():
            all_of(y_out, n - 1, y_send.at[it])

    def forward(it, result):
        x_in = x_ins[it]

        @pl.when(inner)
        def _():
            all_of(x_in, n - 3, x_recv.at[it])

        @pl.when(outer)
        def _():
            all_of(x_in, n - 1, x_recv.at[it])

        def one(q, carry):
            total, key = carry
            left, right, left_at, right_at = tile_pair(f_seat, q)
            stack = jnp.concatenate([tiles[left], tiles[right]], axis=1)
            blocks = jnp.concatenate([x_in[peer_of[left_at]], x_in[peer_of[right_at]]], axis=0)
            product = jnp.dot(stack, blocks, preferred_element_type=jnp.float32)
            new_key = row_of[left_at]
            total = total * (new_key == key).astype(jnp.float32) + product
            f_sums[q] = total
            return total, new_key

        lax.fori_loop(0, f_slots, one, (zero_sum, jnp.int32(-1)), unroll=UNROLL)

        def settle(b, carry):
            total = source[b].astype(jnp.float32) + f_sums[seat(tile_at, f_last, b, f_slots)]
            scale = lax.rsqrt(jnp.mean(total * total, axis=-1, keepdims=True) + epsilon)
            result[b] = (total * scale).astype(jnp.bfloat16)
            return carry

        lax.fori_loop(0, rows, settle, 0)

    def gather(y_in, first, key_of):
        def one(k, carry):
            total, key = carry
            sender = seat(part_at, first, k, n - 1)
            new_key = key_of(sender)
            at = jnp.clip(sender - near_first, 0, half - 1)
            total = total * (new_key == key).astype(jnp.float32) + y_in[at].astype(jnp.float32)
            c_sums[k] = total
            return total, new_key

        lax.fori_loop(0, half, one, (zero_sum, jnp.int32(-1)), unroll=UNROLL)

    def cross_y(it, s):
        first = (1 + s) * part_rows
        all_of(y_gates[it][s], half - 1, y_gate_recv.at[2 * it + s])
        gather(y_gates[it][s], first, lambda d: far_at[d, far_owner[s]])
        if it:
            all_of(y_cross_out.at[s], cap, y_cross_send.at[2 * (it - 1) + s])

        def one(i, carry):
            total = c_sums[seat(part_at, first + c_last, i, half)]
            y_cross_out[s, i] = total.astype(jnp.bfloat16)
            return carry

        lax.fori_loop(0, cap, one, 0)
        push(
            y_cross_out.at[s],
            y_far_ins[it].at[pl.ds(0, cap)],
            y_cross_send.at[2 * it + s],
            y_far_recv.at[it],
            far_owner[s],
        )

    def combine_near(it):
        all_of(y_near_ins[it], half - 1, y_near_recv.at[it])
        gather(y_near_ins[it], 0, asked)

        def settle(b, carry):
            y_mid[b] = y_base[b] + c_sums[seat(part_at, c_last, b, half)]
            return carry

        lax.fori_loop(0, rows, settle, 0)

    def combine_far(it, final):
        y_far = y_far_ins[it]
        all_of(y_far, cap, y_far_recv.at[it])

        def settle(b, carry):
            at = jnp.clip(far_at[far_slot + b, me], 0, cap)
            total = y_mid[b] + y_far[at].astype(jnp.float32)
            scale = lax.rsqrt(jnp.mean(total * total, axis=0, keepdims=True) + epsilon)
            if final:
                target_out[b] = (total * scale).T.astype(jnp.bfloat16)
            else:
                y_now[b] = (total * scale).astype(jnp.bfloat16)
            return carry

        lax.fori_loop(0, rows, settle, 0)

    first_part = 5 * rows // 8

    @pl.when(outer)
    def _():
        send_whole(0, 0, first_part)

    @pl.when(inner)
    def _():
        send_whole(1, 0, rows)

    tile_load.wait()
    backward(0)
    send_parts(0, 1)

    @pl.when(outer)
    def _():
        send_whole(0, first_part, rows - first_part)

    send_parts(0, 0)
    all_of(need_all, n - 1, need_recv.at[0])
    need_load = pltpu.make_async_copy(need_all, need_at, load_sem.at[2])
    need_load.start()
    need_load.wait()
    send_near(source, 0)
    send_near_parts(0)
    plan_far()
    plan_parts()

    @pl.when(inner)
    def _():
        cross_y(0, 1)
        relay(0, 0, True)
        relay(0, 1, True)
        cross_y(0, 0)

    forward(0, x_now)
    for s, here in enumerate((outer, inner)):
        pl.when(here)(functools.partial(send_far, x_now, 1, s))
    combine_near(0)
    combine_far(0, False)
    backward(1)
    sent_parts(0)
    send_parts(1, 1)
    send_parts(1, 0)
    send_near(x_now, 1)

    @pl.when(outer)
    def _():
        send_near_parts(1)

    @pl.when(inner)
    def _():
        relay(1, 0, False)
        send_near_parts(1)
        cross_y(1, 1)
        relay(1, 1, False)
        cross_y(1, 0)

    forward(1, source_out)
    combine_near(1)
    combine_far(1, True)

    all_of(need_all, n - 1, need_send.at[0])
    all_of(x_far_out, cap, gate_send.at[1])
    all_of(x_ins[0], half - 1, x_send.at[ITERS - 1])
    sent_parts(ITERS - 1)

    all_of(gates[0][0], rows, gate_send.at[0])

    @pl.when(inner)
    def _():
        for s in range(2):
            all_of(x_ins[0], half - 1, relay_send.at[2 * (ITERS - 1) + s])
            all_of(y_cross_out.at[s], cap, y_cross_send.at[2 * (ITERS - 1) + s])


def whole_exchange(source, target, tile_values, tile_rows, tile_peers, need_list, tile_count):
    n = lax.axis_size("rows")
    tiles_here, side, _ = tile_values.shape
    width = source.shape[1]
    rows = source.shape[0] // side
    f_slots = slots_for(tiles_here, rows)
    b_slots = slots_for(tiles_here, n)
    tile_plan = (
        lanes_for(2 * f_slots) + lanes_for(rows) + lanes_for(2 * b_slots) + lanes_for(n)
    ) // 128
    part_plan = (lanes_for(n) + lanes_for(rows)) // 128
    block = (side, width)
    vmem = pl.BlockSpec(memory_space=pltpu.VMEM)
    smem = pl.BlockSpec(memory_space=pltpu.SMEM)
    source_now, target_now = pl.pallas_call(
        functools.partial(general, n, f_slots, b_slots),
        out_shape=[pltpu.VMEM((rows,) + block, jnp.bfloat16)] * 2,
        in_specs=[smem] * 3 + [vmem] * 3 + [pl.BlockSpec(memory_space=pltpu.HBM)] * 3,
        out_specs=[vmem, vmem],
        scratch_shapes=[
            pltpu.VMEM((ITERS, n) + block, jnp.bfloat16),
            [pltpu.VMEM((n,) + block, jnp.bfloat16)] * ITERS,
            pltpu.VMEM((ITERS, n) + block, jnp.bfloat16),
            [pltpu.VMEM((n,) + block, jnp.bfloat16)] * ITERS,
            pltpu.VMEM((rows,) + block, jnp.bfloat16),
            pltpu.VMEM((rows,) + block, jnp.bfloat16),
            pltpu.VMEM((rows,) + block, jnp.float32),
            pltpu.VMEM((f_slots + 1,) + block, jnp.float32),
            pltpu.VMEM((b_slots + 1,) + block, jnp.bfloat16),
            pltpu.VMEM((n + 1,) + block, jnp.float32),
            pltpu.VMEM((rows,) + block, jnp.bfloat16),
            pltpu.VMEM((rows,) + block, jnp.bfloat16),
            pltpu.VMEM((tiles_here + 1, side, side), jnp.bfloat16),
            pltpu.VMEM((n, 1, n), jnp.int32),
            pltpu.SMEM((n, 1, n), jnp.int32),
            pltpu.VMEM((tile_plan, 128), jnp.int32),
            pltpu.SMEM((tile_plan, 128), jnp.int32),
            pltpu.VMEM((part_plan, 128), jnp.int32),
            pltpu.SMEM((part_plan, 128), jnp.int32),
            pltpu.SemaphoreType.DMA((2 * ITERS,)),
            pltpu.SemaphoreType.DMA((2 * ITERS,)),
            pltpu.SemaphoreType.DMA((1,)),
            pltpu.SemaphoreType.DMA((1,)),
            pltpu.SemaphoreType.DMA((6,)),
        ],
        compiler_params=pltpu.CompilerParams(
            collective_id=1, has_side_effects=True, vmem_limit_bytes=65000000
        ),
    )(
        tile_rows,
        tile_peers,
        tile_count,
        tile_rows.reshape(1, -1),
        tile_peers.reshape(1, -1),
        need_list,
        source.reshape((rows,) + block),
        target.reshape((rows,) + block),
        tile_values,
    )
    return source_now.reshape(-1, width), target_now.reshape(-1, width)


def shards(source, target, tile_values, tile_rows, tile_peers, need_list, tile_count):
    n = lax.axis_size("rows")
    tiles_here, side, _ = tile_values.shape
    width = source.shape[1]
    rows = source.shape[0] // side
    half, lanes = n // 2, lanes_for(n)
    cap = min(rows, 13)
    f_slots = slots_for(tiles_here, rows)
    b_slots = slots_for(tiles_here, n)
    tile_plan = (
        lanes_for(2 * f_slots) + lanes_for(rows) + lanes_for(2 * b_slots) + lanes_for(n)
    ) // 128
    part_plan = 3 * (lanes_for(n) + lanes_for(rows)) // 128
    far_plan = n + 2 * rows
    block = (side, width)
    vmem = pl.BlockSpec(memory_space=pltpu.VMEM)
    smem = pl.BlockSpec(memory_space=pltpu.SMEM)
    source_now, target_now, over = pl.pallas_call(
        functools.partial(fast, n, cap, f_slots, b_slots),
        out_shape=[pltpu.VMEM((rows,) + block, jnp.bfloat16)] * 2
        + [jax.ShapeDtypeStruct((1, 1), jnp.int32)],
        in_specs=[smem] * 3 + [vmem] * 3 + [pl.BlockSpec(memory_space=pltpu.HBM)] * 3,
        out_specs=[vmem] * 3,
        scratch_shapes=[
            pltpu.VMEM((half,) + block, jnp.bfloat16),
            pltpu.VMEM((cap,) + block, jnp.bfloat16),
            [pltpu.VMEM((n,) + block, jnp.bfloat16)] * ITERS,
            [[pltpu.VMEM((rows,) + block, jnp.bfloat16)] * 2] * ITERS,
            pltpu.VMEM((2, half) + block, jnp.bfloat16),
            pltpu.VMEM((n,) + block, jnp.bfloat16),
            [pltpu.VMEM((half,) + block, jnp.bfloat16)] * ITERS,
            [[pltpu.VMEM((half,) + block, jnp.bfloat16)] * 2] * ITERS,
            pltpu.VMEM((2, cap) + block, jnp.bfloat16),
            [pltpu.VMEM((cap + 1,) + block, jnp.bfloat16)] * ITERS,
            pltpu.VMEM((rows,) + block, jnp.bfloat16),
            pltpu.VMEM((rows,) + block, jnp.bfloat16),
            pltpu.VMEM((rows,) + block, jnp.float32),
            pltpu.VMEM((rows,) + block, jnp.float32),
            pltpu.VMEM((f_slots + 1,) + block, jnp.float32),
            pltpu.VMEM((b_slots + 1,) + block, jnp.bfloat16),
            pltpu.VMEM((half + 1,) + block, jnp.float32),
            pltpu.VMEM((rows,) + block, jnp.bfloat16),
            pltpu.VMEM((rows,) + block, jnp.bfloat16),
            pltpu.VMEM((tiles_here + 1, side, side), jnp.bfloat16),
            pltpu.VMEM((1, lanes), jnp.int32),
            pltpu.VMEM((n, 1, lanes), jnp.int32),
            pltpu.SMEM((n, 1, lanes), jnp.int32),
            pltpu.VMEM((tile_plan, 128), jnp.int32),
            pltpu.SMEM((tile_plan, 128), jnp.int32),
            pltpu.VMEM((part_plan, 128), jnp.int32),
            pltpu.SMEM((part_plan, 128), jnp.int32),
            pltpu.VMEM((far_plan, lanes), jnp.int32),
            pltpu.SMEM((far_plan, lanes), jnp.int32),
            pltpu.SemaphoreType.DMA((ITERS,)),
            pltpu.SemaphoreType.DMA((ITERS,)),
            pltpu.SemaphoreType.DMA((ITERS,)),
            pltpu.SemaphoreType.DMA((2 * ITERS,)),
            pltpu.SemaphoreType.DMA((2 * ITERS,)),
            pltpu.SemaphoreType.DMA((ITERS,)),
            pltpu.SemaphoreType.DMA((ITERS,)),
            pltpu.SemaphoreType.DMA((2 * ITERS,)),
            pltpu.SemaphoreType.DMA((2 * ITERS,)),
            pltpu.SemaphoreType.DMA((ITERS,)),
            pltpu.SemaphoreType.DMA((1,)),
            pltpu.SemaphoreType.DMA((1,)),
            pltpu.SemaphoreType.DMA((7,)),
        ],
        compiler_params=pltpu.CompilerParams(
            collective_id=0, has_side_effects=True, vmem_limit_bytes=65000000
        ),
    )(
        tile_rows,
        tile_peers,
        tile_count,
        tile_rows.reshape(1, -1),
        tile_peers.reshape(1, -1),
        need_list,
        source.reshape((rows,) + block),
        target.reshape((rows,) + block),
        tile_values,
    )
    source_now, target_now = source_now.reshape(-1, width), target_now.reshape(-1, width)
    return lax.cond(
        over.reshape(()) > 0,
        lambda: whole_exchange(
            source, target, tile_values, tile_rows, tile_peers, need_list, tile_count
        ),
        lambda: (source_now, target_now),
    )


def solution(mesh):
    return jax.shard_map(
        shards,
        mesh=mesh,
        in_specs=(
            P("rows", None),
            P("rows", None),
            P("rows", None, None),
            P("rows"),
            P("rows"),
            P("rows", None),
            P("rows"),
        ),
        out_specs=(P("rows", None), P("rows", None)),
        check_vma=False,
    )
```

```python
import functools

import jax
import jax.numpy as jnp
from jax import lax
from jax.experimental import pallas as pl
from jax.experimental.pallas import tpu as pltpu
from jax.sharding import PartitionSpec as P

ITERS = 2
UNROLL = 4
epsilon = 1e-06
MESH = pl.DeviceIdType.MESH


def lanes_for(count):
    return -(-count // 128) * 128


def index_along(shape, axis):
    return lax.broadcasted_iota(jnp.int32, shape, axis).astype(jnp.float32)


def place_groups(keys, groups, per_slot, slots, out, seat_row, last_row):
    items, lanes = keys.shape[1], lanes_for(groups)
    key = jnp.broadcast_to(keys, (items, items))
    key_down = jnp.broadcast_to(keys, (lanes_for(items), items)).T
    before = (key_down[:, :items] == key) & (
        index_along((items, items), 1) < index_along((items, items), 0)
    )
    rank = jnp.sum(before.astype(jnp.float32), axis=1, keepdims=True)
    lane = index_along((items, lanes), 1)
    member = (jnp.broadcast_to(key_down[:, :1], (items, lanes)) == lane).astype(jnp.float32)
    count = jnp.sum(member, axis=0, keepdims=True)
    used = jnp.floor((count + (per_slot - 1)) * (1.0 / per_slot))
    used_down = jnp.broadcast_to(used, (lanes, lanes)).T
    earlier = (index_along((lanes, lanes), 0) < index_along((lanes, lanes), 1)).astype(jnp.float32)
    start = jnp.sum(used_down * earlier, axis=0, keepdims=True)
    last = jnp.where(used > 0, start + used - 1, float(slots))
    first = jnp.sum(member * start, axis=1, keepdims=True)
    place = jnp.where(key_down[:, :1] >= 0, per_slot * first + rank, -1.0)
    seats = lanes_for(slots * per_slot)
    for chunk in range(seats // 128):
        hot = jnp.broadcast_to(place, (items, 128)) == index_along((items, 128), 1) + 128 * chunk
        item = jnp.where(hot, index_along((items, 128), 0) - items, 0.0)
        chosen = items + jnp.sum(item, axis=0, keepdims=True)
        out[pl.ds(seat_row + chunk, 1), :] = chosen.astype(jnp.int32)
    for chunk in range(lanes // 128):
        out[pl.ds(last_row + chunk, 1), :] = last[:, 128 * chunk : 128 * (chunk + 1)].astype(
            jnp.int32
        )


def slots_for(items, groups):
    pairs = (items + min(items, groups)) // 2
    return -(-pairs // UNROLL) * UNROLL


def read_peers(peer_keys, lanes):
    items = peer_keys.shape[1]
    key_down = jnp.broadcast_to(peer_keys, (lanes_for(items), items)).T
    member = jnp.broadcast_to(key_down[:, :1], (items, lanes)) == index_along((items, lanes), 1)
    return jnp.sum(member.astype(jnp.float32), axis=0, keepdims=True)


def general(
    n,
    f_slots,
    b_slots,
    row_of,
    peer_of,
    live_count,
    rows_lane,
    peers_lane,
    need,
    source_hbm,
    target_hbm,
    tiles_hbm,
    source_out,
    target_out,
    x_out,
    x_ins,
    y_out,
    y_ins,
    x_now,
    y_now,
    y_base,
    f_sums,
    b_sums,
    c_sums,
    source,
    target,
    tiles,
    need_all,
    need_at,
    tile_plan,
    tile_at,
    part_plan,
    part_at,
    send_sem,
    recv_sem,
    need_send,
    need_recv,
    load_sem,
):
    me = lax.axis_index("rows")
    rows, side, width = source.shape
    tile_total = tiles_hbm.shape[0]
    f_seat, f_last = 0, lanes_for(2 * f_slots) // 128
    b_seat = f_last + lanes_for(rows) // 128
    b_last = b_seat + lanes_for(2 * b_slots) // 128
    c_last = lanes_for(n) // 128

    barrier = pltpu.get_barrier_semaphore()

    def greet(k, carry):
        pl.semaphore_signal(
            barrier, inc=1, device_id=(lax.rem(me + k, n),), device_id_type=MESH
        )
        return carry

    lax.fori_loop(1, n, greet, 0)
    source_load = pltpu.make_async_copy(source_hbm, source, load_sem.at[5])
    source_load.start()
    target_load = pltpu.make_async_copy(target_hbm, target, load_sem.at[0])
    target_load.start()
    tile_load = pltpu.make_async_copy(tiles_hbm, tiles.at[pl.ds(0, tile_total)], load_sem.at[1])
    tile_load.start()

    zero_block = jnp.zeros((side, width), jnp.bfloat16)
    zero_sum = jnp.zeros((side, width), jnp.float32)
    tiles[tile_total] = jnp.zeros((side, side), jnp.bfloat16)
    f_sums[f_slots] = zero_sum
    b_sums[b_slots] = zero_block
    c_sums[n] = zero_sum
    need_all[me] = need[...]
    pl.semaphore_wait(barrier, n - 1)

    def ask(k, carry):
        pltpu.make_async_remote_copy(
            src_ref=need,
            dst_ref=need_all.at[me],
            send_sem=need_send.at[0],
            recv_sem=need_recv.at[0],
            device_id=(lax.rem(me + k, n),),
            device_id_type=MESH,
        ).start()
        return carry

    lax.fori_loop(1, n, ask, 0)

    def turn(b, carry):
        flipped = target[b].astype(jnp.float32).T
        y_base[b] = flipped
        y_now[b] = flipped.astype(jnp.bfloat16)
        return carry

    def plan_tiles():
        live = lax.broadcasted_iota(jnp.int32, (1, tile_total), 1) < live_count[0]
        row_keys = jnp.where(live, rows_lane[...], -1).astype(jnp.float32)
        peer_keys = jnp.where(live, peers_lane[...], -1).astype(jnp.float32)
        place_groups(row_keys, rows, 2, f_slots, tile_plan, f_seat, f_last)
        place_groups(peer_keys, n, 2, b_slots, tile_plan, b_seat, b_last)
        load = pltpu.make_async_copy(tile_plan, tile_at, load_sem.at[3])
        load.start()
        load.wait()

    def plan_parts():
        table = need_all[...].reshape(n, need_all.shape[2]).astype(jnp.float32)
        mine = index_along(table.shape, 1) == me.astype(jnp.float32)
        wanted = jnp.sum(jnp.where(mine, table, 0.0), axis=1, keepdims=True)
        keys = jnp.broadcast_to(wanted, (n, 128)).T[:1]
        place_groups(keys, rows, 1, n, part_plan, 0, c_last)
        load = pltpu.make_async_copy(part_plan, part_at, load_sem.at[4])
        load.start()
        load.wait()

    def seat(table, first, index, top):
        return jnp.clip(table[first + index // 128, index % 128], 0, top)

    def tile_pair(first, q):
        left = seat(tile_at, first, 2 * q, tile_total)
        right = seat(tile_at, first, 2 * q + 1, tile_total)
        return left, right, jnp.minimum(left, tile_total - 1), jnp.minimum(right, tile_total - 1)

    def asked(d):
        return jnp.clip(need_at[d, 0, me], 0, rows - 1)

    def send(out, inn, phase, it, fill):
        def one(k, carry):
            peer = lax.rem(me + k, n)
            out[it, peer] = fill(peer)
            pltpu.make_async_remote_copy(
                src_ref=out.at[it, peer],
                dst_ref=inn.at[me],
                send_sem=send_sem.at[phase],
                recv_sem=recv_sem.at[phase],
                device_id=(peer,),
                device_id_type=MESH,
            ).start()
            return carry

        lax.fori_loop(1, n, one, 0)
        inn[me] = fill(me)

    def all_of(buffer, sem):
        view = buffer.at[pl.ds(0, n - 1)]
        pltpu.make_async_copy(view, view, sem).wait()

    def send_x(blocks, it):
        send(x_out, x_ins[it], 2 * it, it, lambda p: blocks[asked(p)])

    def backward(it):
        def one(q, carry):
            total, key = carry
            left, right, left_at, right_at = tile_pair(b_seat, q)
            flipped = jnp.concatenate([y_now[row_of[left_at]], y_now[row_of[right_at]]], axis=1)
            stack = jnp.concatenate([tiles[left], tiles[right]], axis=0)
            product = jnp.dot(flipped, stack, preferred_element_type=jnp.float32)
            new_key = peer_of[left_at]
            total = total * (new_key == key).astype(jnp.float32) + product
            b_sums[q] = total.astype(jnp.bfloat16)
            return total, new_key

        lax.fori_loop(0, b_slots, one, (zero_sum, jnp.int32(-1)), unroll=UNROLL)
        send(y_out, y_ins[it], 2 * it + 1, it, lambda p: b_sums[seat(tile_at, b_last, p, b_slots)])

    def forward(it, result):
        x_in = x_ins[it]
        all_of(x_in, recv_sem.at[2 * it])

        def one(q, carry):
            total, key = carry
            left, right, left_at, right_at = tile_pair(f_seat, q)
            stack = jnp.concatenate([tiles[left], tiles[right]], axis=1)
            blocks = jnp.concatenate([x_in[peer_of[left_at]], x_in[peer_of[right_at]]], axis=0)
            product = jnp.dot(stack, blocks, preferred_element_type=jnp.float32)
            new_key = row_of[left_at]
            total = total * (new_key == key).astype(jnp.float32) + product
            f_sums[q] = total
            return total, new_key

        lax.fori_loop(0, f_slots, one, (zero_sum, jnp.int32(-1)), unroll=UNROLL)

        def settle(b, carry):
            total = source[b].astype(jnp.float32) + f_sums[seat(tile_at, f_last, b, f_slots)]
            scale = lax.rsqrt(jnp.mean(total * total, axis=-1, keepdims=True) + epsilon)
            result[b] = (total * scale).astype(jnp.bfloat16)
            return carry

        lax.fori_loop(0, rows, settle, 0)

    def combine(it, final):
        y_in = y_ins[it]
        all_of(y_in, recv_sem.at[2 * it + 1])

        def one(k, carry):
            total, key = carry
            sender = seat(part_at, 0, k, n - 1)
            new_key = asked(sender)
            total = total * (new_key == key).astype(jnp.float32) + y_in[sender].astype(jnp.float32)
            c_sums[k] = total
            return total, new_key

        lax.fori_loop(0, n, one, (zero_sum, jnp.int32(-1)), unroll=UNROLL)

        def settle(b, carry):
            total = y_base[b] + c_sums[seat(part_at, c_last, b, n)]
            scale = lax.rsqrt(jnp.mean(total * total, axis=0, keepdims=True) + epsilon)
            if final:
                target_out[b] = (total * scale).T.astype(jnp.bfloat16)
            else:
                y_now[b] = (total * scale).astype(jnp.bfloat16)
            return carry

        lax.fori_loop(0, rows, settle, 0)

    all_of(need_all, need_recv.at[0])
    need_load = pltpu.make_async_copy(need_all, need_at, load_sem.at[2])
    need_load.start()
    need_load.wait()
    source_load.wait()
    send_x(source, 0)
    plan_tiles()
    target_load.wait()
    lax.fori_loop(0, rows, turn, 0)
    tile_load.wait()
    backward(0)
    plan_parts()
    for it in range(ITERS):
        final = it == ITERS - 1
        forward(it, source_out if final else x_now)
        if not final:
            send_x(x_now, it + 1)
        combine(it, final)
        if not final:
            backward(it + 1)
    all_of(need_all, need_send.at[0])
    for it in range(ITERS):
        all_of(x_out.at[it], send_sem.at[2 * it])
        all_of(y_out.at[it], send_sem.at[2 * it + 1])


def fast(
    n,
    cap,
    f_slots,
    b_slots,
    row_of,
    peer_of,
    live_count,
    rows_lane,
    peers_lane,
    need,
    source_hbm,
    target_hbm,
    tiles_hbm,
    source_out,
    target_out,
    over_out,
    x_near_out,
    x_far_out,
    x_ins,
    hubs,
    hub_out,
    gates,
    relay_out,
    y_out,
    y_near_ins,
    y_gates,
    y_cross_out,
    y_far_ins,
    x_now,
    y_now,
    y_base,
    y_mid,
    f_sums,
    b_sums,
    c_sums,
    source,
    target,
    tiles,
    need_mine,
    need_all,
    need_at,
    tile_plan,
    tile_at,
    part_plan,
    part_at,
    far_plan,
    far_at,
    x_send,
    x_recv,
    hub_send,
    hub_recv,
    spoke_send,
    gate_send,
    gate_recv,
    relay_send,
    y_send,
    y_near_recv,
    y_gate_recv,
    y_cross_send,
    y_far_recv,
    need_send,
    need_recv,
    load_sem,
):
    me = lax.axis_index("rows")
    rows, side, width = source.shape
    tile_total = tiles_hbm.shape[0]
    lanes = lanes_for(n)
    half, plane = n // 2, n // 4
    upper = me // half
    near_first, far_first = upper * half, (1 - upper) * half
    spot, column = me % half, me % plane
    inner = me // plane == 1 + upper
    outer = jnp.logical_not(inner)
    far_gate = (2 - upper) * plane + column
    near_gates = (1 + upper) * plane
    mine_first = me - column
    other_first = 2 * near_first + plane - mine_first
    near_gate = near_gates + column
    outer_owner = 3 * upper * plane + column
    far_planes = (3 * (1 - upper) * plane, (2 - upper) * plane)
    far_owner = tuple(first + column for first in far_planes)
    f_seat, f_last = 0, lanes_for(2 * f_slots) // 128
    b_seat = f_last + lanes_for(rows) // 128
    b_last = b_seat + lanes_for(2 * b_slots) // 128
    c_last = lanes_for(n) // 128
    part_rows = c_last + lanes_for(rows) // 128
    far_list = n
    far_slot = n + rows

    barrier = pltpu.get_barrier_semaphore()

    def greet(k, carry):
        pl.semaphore_signal(
            barrier, inc=1, device_id=(lax.rem(me + k, n),), device_id_type=MESH
        )
        return carry

    lax.fori_loop(1, n, greet, 0)
    source_load = pltpu.make_async_copy(source_hbm, source, load_sem.at[5])
    source_load.start()
    target_load = pltpu.make_async_copy(target_hbm, target, load_sem.at[0])
    target_load.start()
    tile_load = pltpu.make_async_copy(tiles_hbm, tiles.at[pl.ds(0, tile_total)], load_sem.at[1])
    tile_load.start()

    live = lax.broadcasted_iota(jnp.int32, (1, tile_total), 1) < live_count[0]
    row_keys = jnp.where(live, rows_lane[...], -1).astype(jnp.float32)
    peer_keys = jnp.where(live, peers_lane[...], -1).astype(jnp.float32)
    read = read_peers(peer_keys, lanes)
    need_mine[...] = jnp.full((1, lanes), -1, jnp.int32)
    need_mine[:, :n] = jnp.where(read[:, :n] > 0, need[...], -1)
    zero_block = jnp.zeros((side, width), jnp.bfloat16)
    zero_sum = jnp.zeros((side, width), jnp.float32)
    tiles[tile_total] = jnp.zeros((side, side), jnp.bfloat16)
    f_sums[f_slots] = zero_sum
    b_sums[b_slots] = zero_block
    c_sums[half] = zero_sum
    for it in range(ITERS):
        y_far_ins[it][cap] = zero_block
    need_all[me] = need_mine[...]
    def turn(b, carry):
        flipped = target[b].astype(jnp.float32).T
        y_base[b] = flipped
        y_now[b] = flipped.astype(jnp.bfloat16)
        return carry

    def plan_tiles():
        place_groups(row_keys, rows, 2, f_slots, tile_plan, f_seat, f_last)
        place_groups(peer_keys, n, 2, b_slots, tile_plan, b_seat, b_last)
        load = pltpu.make_async_copy(tile_plan, tile_at, load_sem.at[3])
        load.start()
        load.wait()

    plan_tiles()
    target_load.wait()
    lax.fori_loop(0, rows, turn, 0)
    source_load.wait()
    pl.semaphore_wait(barrier, n - 1)

    def push(src, dst, send_sem, recv_sem, peer):
        pltpu.make_async_remote_copy(
            src_ref=src,
            dst_ref=dst,
            send_sem=send_sem,
            recv_sem=recv_sem,
            device_id=(peer,),
            device_id_type=MESH,
        ).start()

    def all_of(buffer, count, sem):
        view = buffer.at[pl.ds(0, count)]
        pltpu.make_async_copy(view, view, sem).wait()

    def ask(k, carry):
        peer = lax.rem(me + k, n)
        push(need_mine, need_all.at[me], need_send.at[0], need_recv.at[0], peer)
        return carry

    lax.fori_loop(1, n, ask, 0)

    def needs():
        return need_all[...].reshape(n, lanes).astype(jnp.float32)

    def plan_far():
        table = needs()
        early = index_along((1, lanes), 1) < half
        before = jnp.zeros((1, lanes), jnp.float32)
        place = jnp.zeros((n, lanes), jnp.float32)
        listed = jnp.zeros((rows, lanes), jnp.float32)
        for b in range(rows):
            hit = (table == b).astype(jnp.float32)
            low = jnp.max(hit[:half], axis=0, keepdims=True)
            high = jnp.max(hit[half:], axis=0, keepdims=True)
            used = jnp.where(early, high, low)
            place = place + hit * before
            chosen = jnp.where(used > 0, before, -1.0)
            listed = jnp.where(index_along((rows, lanes), 0) == chosen, float(b), listed)
            far_plan[pl.ds(far_slot + b, 1), :] = jnp.where(used > 0, before, float(cap)).astype(
                jnp.int32
            )
            before = before + used
        far_plan[pl.ds(0, n), :] = place.astype(jnp.int32)
        far_plan[pl.ds(far_list, rows), :] = listed.astype(jnp.int32)
        worst = jnp.max(before, axis=1, keepdims=True)
        over_out[...] = (worst > cap).astype(jnp.int32)
        load = pltpu.make_async_copy(far_plan, far_at, load_sem.at[6])
        load.start()
        load.wait()

    def plan_parts():
        table = needs()
        sender = index_along((n, lanes), 0)
        lane = index_along((n, lanes), 1)
        near = (sender >= near_first.astype(jnp.float32)) & (
            sender < (near_first + half).astype(jnp.float32)
        )
        known = near & (table >= 0)
        place = far_plan[pl.ds(0, n), :].astype(jnp.float32)

        def column_of(values, at):
            mine = lane == at.astype(jnp.float32)
            column = jnp.sum(jnp.where(mine, values, 0.0), axis=1, keepdims=True)
            return jnp.broadcast_to(column, (n, 128)).T[:1]

        def plan(values, at, first):
            keys = column_of(jnp.where(known, values, -1.0), at)
            place_groups(keys, rows, 1, half, part_plan, first, first + c_last)

        plan(table, me, 0)
        for s in range(2):
            plan(place, far_owner[s], (1 + s) * part_rows)
        load = pltpu.make_async_copy(part_plan, part_at, load_sem.at[4])
        load.start()
        load.wait()

    def seat(table, first, index, top):
        return jnp.clip(table[first + index // 128, index % 128], 0, top)

    def tile_pair(first, q):
        left = seat(tile_at, first, 2 * q, tile_total)
        right = seat(tile_at, first, 2 * q + 1, tile_total)
        return left, right, jnp.minimum(left, tile_total - 1), jnp.minimum(right, tile_total - 1)

    def asked(d):
        return jnp.clip(need_at[d, 0, me], 0, rows - 1)

    def to_plane(one, first, low):
        def step(k, carry):
            one(first + lax.rem(column + k, plane), plane + k if low else k)
            return carry

        lax.fori_loop(low, plane, step, 0)

    def to_half(one):
        to_plane(one, other_first, 0)
        to_plane(one, mine_first, 1)

    def send_near(blocks, it):
        x_in = x_ins[it]

        def one(peer, k):
            x_near_out[k] = blocks[asked(peer)]
            push(x_near_out.at[k], x_in.at[me], x_send.at[it], x_recv.at[it], peer)

        if it:
            sent_near(it - 1)

        @pl.when(inner)
        def _():
            to_half(one)

        @pl.when(outer)
        def _():
            to_plane(one, mine_first, 1)

        x_in[me] = blocks[asked(me)]

    def sent_near(it):
        @pl.when(inner)
        def _():
            all_of(x_near_out, half - 1, x_send.at[it])

        @pl.when(outer)
        def _():
            all_of(x_near_out, plane - 1, x_send.at[it])

    def send_hub(blocks, it):
        push(blocks, hubs[it], hub_send.at[it], hub_recv.at[it], near_gate)

    def send_far(blocks, it, s, owner):
        if it:
            sent_far(it - 1, s)

        def one(i, carry):
            x_far_out[s, i] = blocks[jnp.clip(far_at[far_list + i, owner], 0, rows - 1)]
            return carry

        lax.fori_loop(0, cap, one, 0)
        push(
            x_far_out.at[s],
            gates[it][s].at[pl.ds(0, cap)],
            gate_send.at[2 * it + s],
            gate_recv.at[2 * it + s],
            far_gate,
        )

    def sent_far(it, s):
        whole = it == 0 and s == 1
        all_of(gates[it][s], rows if whole else cap, gate_send.at[2 * it + s])

    def hub(it):
        held, x_in = hubs[it], x_ins[it]
        all_of(held, rows, hub_recv.at[it])
        send_far(held, it, 0, outer_owner)
        if it:
            all_of(hub_out, plane - 1, spoke_send.at[it - 1])

        def block(d):
            return held[jnp.clip(need_at[d, 0, outer_owner], 0, rows - 1)]

        def one(k, carry):
            peer = near_gates + lax.rem(column + k, plane)
            hub_out[k] = block(peer)
            push(
                hub_out.at[k], x_in.at[outer_owner], spoke_send.at[it], x_recv.at[it], peer
            )
            return carry

        lax.fori_loop(1, plane, one, 0)
        x_in[outer_owner] = block(me)

    def relay(it, s, whole):
        gate, x_in, owner = gates[it][s], x_ins[it], far_owner[s]
        if it:
            all_of(x_in, half - 1, relay_send.at[2 * (it - 1) + s])
        all_of(gate, rows if whole else cap, gate_recv.at[2 * it + s])

        def block(d):
            at = need_at[d, 0, owner] if whole else far_at[d, owner]
            return gate[jnp.clip(at, 0, (rows if whole else cap) - 1)]

        def one(peer, k):
            relay_out[s, k] = block(peer)
            push(
                relay_out.at[s, k],
                x_in.at[owner],
                relay_send.at[2 * it + s],
                x_recv.at[it],
                peer,
            )

        to_half(one)
        x_in[owner] = block(me)

    def backward(it):
        def one(q, carry):
            total, key = carry
            left, right, left_at, right_at = tile_pair(b_seat, q)
            flipped = jnp.concatenate([y_now[row_of[left_at]], y_now[row_of[right_at]]], axis=1)
            stack = jnp.concatenate([tiles[left], tiles[right]], axis=0)
            product = jnp.dot(flipped, stack, preferred_element_type=jnp.float32)
            new_key = peer_of[left_at]
            total = total * (new_key == key).astype(jnp.float32) + product
            b_sums[q] = total.astype(jnp.bfloat16)
            return total, new_key

        lax.fori_loop(0, b_slots, one, (zero_sum, jnp.int32(-1)), unroll=UNROLL)

    def part(peer):
        return b_sums[seat(tile_at, b_last, peer, b_slots)]

    def send_parts(it, s):
        gate_in = y_gates[it][s]

        def one(k, carry):
            gate = lax.rem(column + k, plane)
            peer = far_planes[s] + gate
            y_out[peer] = part(peer)
            push(
                y_out.at[peer],
                gate_in.at[spot],
                y_send.at[it],
                y_gate_recv.at[2 * it + s],
                near_gates + gate,
            )
            return carry

        @pl.when(outer)
        def _():
            one(0, 0)

        @pl.when(inner)
        def _():
            gate_in[spot] = part(far_owner[s])

        lax.fori_loop(1, plane, one, 0)

    def send_near_parts(it):
        def one(peer, k):
            y_out[peer] = part(peer)
            push(y_out.at[peer], y_near_ins[it].at[spot], y_send.at[it], y_near_recv.at[it], peer)

        to_half(one)
        y_near_ins[it][spot] = part(me)

    def sent_parts(it):
        @pl.when(inner)
        def _():
            all_of(y_out, n - 3, y_send.at[it])

        @pl.when(outer)
        def _():
            all_of(y_out, n - 1, y_send.at[it])

    def forward(it, result):
        x_in = x_ins[it]

        @pl.when(inner)
        def _():
            all_of(x_in, n - 4, x_recv.at[it])

        @pl.when(outer)
        def _():
            all_of(x_in, n - 1, x_recv.at[it])

        def one(q, carry):
            total, key = carry
            left, right, left_at, right_at = tile_pair(f_seat, q)
            stack = jnp.concatenate([tiles[left], tiles[right]], axis=1)
            blocks = jnp.concatenate([x_in[peer_of[left_at]], x_in[peer_of[right_at]]], axis=0)
            product = jnp.dot(stack, blocks, preferred_element_type=jnp.float32)
            new_key = row_of[left_at]
            total = total * (new_key == key).astype(jnp.float32) + product
            f_sums[q] = total
            return total, new_key

        lax.fori_loop(0, f_slots, one, (zero_sum, jnp.int32(-1)), unroll=UNROLL)

        def settle(b, carry):
            total = source[b].astype(jnp.float32) + f_sums[seat(tile_at, f_last, b, f_slots)]
            scale = lax.rsqrt(jnp.mean(total * total, axis=-1, keepdims=True) + epsilon)
            result[b] = (total * scale).astype(jnp.bfloat16)
            return carry

        lax.fori_loop(0, rows, settle, 0)

    def gather(y_in, first, key_of):
        def one(k, carry):
            total, key = carry
            sender = seat(part_at, first, k, n - 1)
            new_key = key_of(sender)
            at = jnp.clip(sender - near_first, 0, half - 1)
            total = total * (new_key == key).astype(jnp.float32) + y_in[at].astype(jnp.float32)
            c_sums[k] = total
            return total, new_key

        lax.fori_loop(0, half, one, (zero_sum, jnp.int32(-1)), unroll=UNROLL)

    def cross_y(it, s):
        first = (1 + s) * part_rows
        all_of(y_gates[it][s], half - 1, y_gate_recv.at[2 * it + s])
        gather(y_gates[it][s], first, lambda d: far_at[d, far_owner[s]])
        if it:
            all_of(y_cross_out.at[s], cap, y_cross_send.at[2 * (it - 1) + s])

        def one(i, carry):
            total = c_sums[seat(part_at, first + c_last, i, half)]
            y_cross_out[s, i] = total.astype(jnp.bfloat16)
            return carry

        lax.fori_loop(0, cap, one, 0)
        push(
            y_cross_out.at[s],
            y_far_ins[it].at[pl.ds(0, cap)],
            y_cross_send.at[2 * it + s],
            y_far_recv.at[it],
            far_owner[s],
        )

    def combine_near(it):
        all_of(y_near_ins[it], half - 1, y_near_recv.at[it])
        gather(y_near_ins[it], 0, asked)

        def settle(b, carry):
            y_mid[b] = y_base[b] + c_sums[seat(part_at, c_last, b, half)]
            return carry

        lax.fori_loop(0, rows, settle, 0)

    def combine_far(it, final):
        y_far = y_far_ins[it]
        all_of(y_far, cap, y_far_recv.at[it])

        def settle(b, carry):
            at = jnp.clip(far_at[far_slot + b, me], 0, cap)
            total = y_mid[b] + y_far[at].astype(jnp.float32)
            scale = lax.rsqrt(jnp.mean(total * total, axis=0, keepdims=True) + epsilon)
            if final:
                target_out[b] = (total * scale).T.astype(jnp.bfloat16)
            else:
                y_now[b] = (total * scale).astype(jnp.bfloat16)
            return carry

        lax.fori_loop(0, rows, settle, 0)

    def learn_needs():
        all_of(need_all, n - 1, need_recv.at[0])
        need_load = pltpu.make_async_copy(need_all, need_at, load_sem.at[2])
        need_load.start()
        plan_far()
        need_load.wait()

    @pl.when(inner)
    def _():
        push(source, gates[0][1], gate_send.at[1], gate_recv.at[1], far_gate)

    @pl.when(outer)
    def _():
        send_hub(source, 0)

    tile_load.wait()
    backward(0)
    send_parts(0, 1)
    send_parts(0, 0)
    learn_needs()
    send_near(source, 0)
    pl.when(outer)(functools.partial(send_near_parts, 0))
    plan_parts()

    @pl.when(inner)
    def _():
        hub(0)
        relay(0, 1, True)
        cross_y(0, 1)
        relay(0, 0, False)
        send_near_parts(0)
        cross_y(0, 0)

    forward(0, x_now)

    @pl.when(inner)
    def _():
        send_far(x_now, 1, 1, me)

    @pl.when(outer)
    def _():
        send_hub(x_now, 1)

    send_near(x_now, 1)
    combine_near(0)
    combine_far(0, False)
    backward(1)
    sent_parts(0)
    send_parts(1, 1)
    send_parts(1, 0)
    send_near_parts(1)

    @pl.when(inner)
    def _():
        relay(1, 1, False)
        hub(1)
        cross_y(1, 1)
        relay(1, 0, False)
        cross_y(1, 0)

    forward(1, source_out)
    combine_near(1)
    combine_far(1, True)

    all_of(need_all, n - 1, need_send.at[0])
    sent_near(ITERS - 1)
    sent_parts(ITERS - 1)

    @pl.when(outer)
    def _():
        for it in range(ITERS):
            all_of(hubs[it], rows, hub_send.at[it])

    @pl.when(inner)
    def _():
        all_of(hub_out, plane - 1, spoke_send.at[ITERS - 1])
        for s in range(2):
            sent_far(ITERS - 1, s)
            all_of(x_ins[0], half - 1, relay_send.at[2 * (ITERS - 1) + s])
            all_of(y_cross_out.at[s], cap, y_cross_send.at[2 * (ITERS - 1) + s])


def whole_exchange(source, target, tile_values, tile_rows, tile_peers, need_list, tile_count):
    n = lax.axis_size("rows")
    tiles_here, side, _ = tile_values.shape
    width = source.shape[1]
    rows = source.shape[0] // side
    f_slots = slots_for(tiles_here, rows)
    b_slots = slots_for(tiles_here, n)
    tile_plan = (
        lanes_for(2 * f_slots) + lanes_for(rows) + lanes_for(2 * b_slots) + lanes_for(n)
    ) // 128
    part_plan = (lanes_for(n) + lanes_for(rows)) // 128
    block = (side, width)
    vmem = pl.BlockSpec(memory_space=pltpu.VMEM)
    smem = pl.BlockSpec(memory_space=pltpu.SMEM)
    source_now, target_now = pl.pallas_call(
        functools.partial(general, n, f_slots, b_slots),
        out_shape=[pltpu.VMEM((rows,) + block, jnp.bfloat16)] * 2,
        in_specs=[smem] * 3 + [vmem] * 3 + [pl.BlockSpec(memory_space=pltpu.HBM)] * 3,
        out_specs=[vmem, vmem],
        scratch_shapes=[
            pltpu.VMEM((ITERS, n) + block, jnp.bfloat16),
            [pltpu.VMEM((n,) + block, jnp.bfloat16)] * ITERS,
            pltpu.VMEM((ITERS, n) + block, jnp.bfloat16),
            [pltpu.VMEM((n,) + block, jnp.bfloat16)] * ITERS,
            pltpu.VMEM((rows,) + block, jnp.bfloat16),
            pltpu.VMEM((rows,) + block, jnp.bfloat16),
            pltpu.VMEM((rows,) + block, jnp.float32),
            pltpu.VMEM((f_slots + 1,) + block, jnp.float32),
            pltpu.VMEM((b_slots + 1,) + block, jnp.bfloat16),
            pltpu.VMEM((n + 1,) + block, jnp.float32),
            pltpu.VMEM((rows,) + block, jnp.bfloat16),
            pltpu.VMEM((rows,) + block, jnp.bfloat16),
            pltpu.VMEM((tiles_here + 1, side, side), jnp.bfloat16),
            pltpu.VMEM((n, 1, n), jnp.int32),
            pltpu.SMEM((n, 1, n), jnp.int32),
            pltpu.VMEM((tile_plan, 128), jnp.int32),
            pltpu.SMEM((tile_plan, 128), jnp.int32),
            pltpu.VMEM((part_plan, 128), jnp.int32),
            pltpu.SMEM((part_plan, 128), jnp.int32),
            pltpu.SemaphoreType.DMA((2 * ITERS,)),
            pltpu.SemaphoreType.DMA((2 * ITERS,)),
            pltpu.SemaphoreType.DMA((1,)),
            pltpu.SemaphoreType.DMA((1,)),
            pltpu.SemaphoreType.DMA((6,)),
        ],
        compiler_params=pltpu.CompilerParams(
            collective_id=1, has_side_effects=True, vmem_limit_bytes=65000000
        ),
    )(
        tile_rows,
        tile_peers,
        tile_count,
        tile_rows.reshape(1, -1),
        tile_peers.reshape(1, -1),
        need_list,
        source.reshape((rows,) + block),
        target.reshape((rows,) + block),
        tile_values,
    )
    return source_now.reshape(-1, width), target_now.reshape(-1, width)


def shards(source, target, tile_values, tile_rows, tile_peers, need_list, tile_count):
    n = lax.axis_size("rows")
    tiles_here, side, _ = tile_values.shape
    width = source.shape[1]
    rows = source.shape[0] // side
    half, lanes = n // 2, lanes_for(n)
    cap = min(rows, 13)
    f_slots = slots_for(tiles_here, rows)
    b_slots = slots_for(tiles_here, n)
    tile_plan = (
        lanes_for(2 * f_slots) + lanes_for(rows) + lanes_for(2 * b_slots) + lanes_for(n)
    ) // 128
    part_plan = 3 * (lanes_for(n) + lanes_for(rows)) // 128
    far_plan = n + 2 * rows
    block = (side, width)
    vmem = pl.BlockSpec(memory_space=pltpu.VMEM)
    smem = pl.BlockSpec(memory_space=pltpu.SMEM)
    source_now, target_now, over = pl.pallas_call(
        functools.partial(fast, n, cap, f_slots, b_slots),
        out_shape=[pltpu.VMEM((rows,) + block, jnp.bfloat16)] * 2
        + [jax.ShapeDtypeStruct((1, 1), jnp.int32)],
        in_specs=[smem] * 3 + [vmem] * 3 + [pl.BlockSpec(memory_space=pltpu.HBM)] * 3,
        out_specs=[vmem] * 3,
        scratch_shapes=[
            pltpu.VMEM((half,) + block, jnp.bfloat16),
            pltpu.VMEM((2, cap) + block, jnp.bfloat16),
            [pltpu.VMEM((n,) + block, jnp.bfloat16)] * ITERS,
            [pltpu.VMEM((rows,) + block, jnp.bfloat16)] * ITERS,
            pltpu.VMEM((n // 4,) + block, jnp.bfloat16),
            [[pltpu.VMEM((rows,) + block, jnp.bfloat16)] * 2] * ITERS,
            pltpu.VMEM((2, half) + block, jnp.bfloat16),
            pltpu.VMEM((n,) + block, jnp.bfloat16),
            [pltpu.VMEM((half,) + block, jnp.bfloat16)] * ITERS,
            [[pltpu.VMEM((half,) + block, jnp.bfloat16)] * 2] * ITERS,
            pltpu.VMEM((2, cap) + block, jnp.bfloat16),
            [pltpu.VMEM((cap + 1,) + block, jnp.bfloat16)] * ITERS,
            pltpu.VMEM((rows,) + block, jnp.bfloat16),
            pltpu.VMEM((rows,) + block, jnp.bfloat16),
            pltpu.VMEM((rows,) + block, jnp.float32),
            pltpu.VMEM((rows,) + block, jnp.float32),
            pltpu.VMEM((f_slots + 1,) + block, jnp.float32),
            pltpu.VMEM((b_slots + 1,) + block, jnp.bfloat16),
            pltpu.VMEM((half + 1,) + block, jnp.float32),
            pltpu.VMEM((rows,) + block, jnp.bfloat16),
            pltpu.VMEM((rows,) + block, jnp.bfloat16),
            pltpu.VMEM((tiles_here + 1, side, side), jnp.bfloat16),
            pltpu.VMEM((1, lanes), jnp.int32),
            pltpu.VMEM((n, 1, lanes), jnp.int32),
            pltpu.SMEM((n, 1, lanes), jnp.int32),
            pltpu.VMEM((tile_plan, 128), jnp.int32),
            pltpu.SMEM((tile_plan, 128), jnp.int32),
            pltpu.VMEM((part_plan, 128), jnp.int32),
            pltpu.SMEM((part_plan, 128), jnp.int32),
            pltpu.VMEM((far_plan, lanes), jnp.int32),
            pltpu.SMEM((far_plan, lanes), jnp.int32),
            pltpu.SemaphoreType.DMA((ITERS,)),
            pltpu.SemaphoreType.DMA((ITERS,)),
            pltpu.SemaphoreType.DMA((ITERS,)),
            pltpu.SemaphoreType.DMA((ITERS,)),
            pltpu.SemaphoreType.DMA((ITERS,)),
            pltpu.SemaphoreType.DMA((2 * ITERS,)),
            pltpu.SemaphoreType.DMA((2 * ITERS,)),
            pltpu.SemaphoreType.DMA((2 * ITERS,)),
            pltpu.SemaphoreType.DMA((ITERS,)),
            pltpu.SemaphoreType.DMA((ITERS,)),
            pltpu.SemaphoreType.DMA((2 * ITERS,)),
            pltpu.SemaphoreType.DMA((2 * ITERS,)),
            pltpu.SemaphoreType.DMA((ITERS,)),
            pltpu.SemaphoreType.DMA((1,)),
            pltpu.SemaphoreType.DMA((1,)),
            pltpu.SemaphoreType.DMA((7,)),
        ],
        compiler_params=pltpu.CompilerParams(
            collective_id=0, has_side_effects=True, vmem_limit_bytes=65000000
        ),
    )(
        tile_rows,
        tile_peers,
        tile_count,
        tile_rows.reshape(1, -1),
        tile_peers.reshape(1, -1),
        need_list,
        source.reshape((rows,) + block),
        target.reshape((rows,) + block),
        tile_values,
    )
    source_now, target_now = source_now.reshape(-1, width), target_now.reshape(-1, width)
    return lax.cond(
        over.reshape(()) > 0,
        lambda: whole_exchange(
            source, target, tile_values, tile_rows, tile_peers, need_list, tile_count
        ),
        lambda: (source_now, target_now),
    )


def solution(mesh):
    return jax.shard_map(
        shards,
        mesh=mesh,
        in_specs=(
            P("rows", None),
            P("rows", None),
            P("rows", None, None),
            P("rows"),
            P("rows"),
            P("rows", None),
            P("rows"),
        ),
        out_specs=(P("rows", None), P("rows", None)),
        check_vma=False,
    )
```

```python
import functools

import jax
import jax.numpy as jnp
from jax import lax
from jax.experimental import pallas as pl
from jax.experimental.pallas import tpu as pltpu
from jax.sharding import PartitionSpec as P

ITERS = 2
UNROLL = 4
epsilon = 1e-06
MESH = pl.DeviceIdType.MESH


def lanes_for(count):
    return -(-count // 128) * 128


def index_along(shape, axis):
    return lax.broadcasted_iota(jnp.int32, shape, axis).astype(jnp.float32)


def place_groups(keys, groups, per_slot, slots, out, seat_row, last_row):
    items, lanes = keys.shape[1], lanes_for(groups)
    key = jnp.broadcast_to(keys, (items, items))
    key_down = jnp.broadcast_to(keys, (lanes_for(items), items)).T
    before = (key_down[:, :items] == key) & (
        index_along((items, items), 1) < index_along((items, items), 0)
    )
    rank = jnp.sum(before.astype(jnp.float32), axis=1, keepdims=True)
    lane = index_along((items, lanes), 1)
    member = (jnp.broadcast_to(key_down[:, :1], (items, lanes)) == lane).astype(jnp.float32)
    count = jnp.sum(member, axis=0, keepdims=True)
    used = jnp.floor((count + (per_slot - 1)) * (1.0 / per_slot))
    used_down = jnp.broadcast_to(used, (lanes, lanes)).T
    earlier = (index_along((lanes, lanes), 0) < index_along((lanes, lanes), 1)).astype(jnp.float32)
    start = jnp.sum(used_down * earlier, axis=0, keepdims=True)
    last = jnp.where(used > 0, start + used - 1, float(slots))
    first = jnp.sum(member * start, axis=1, keepdims=True)
    place = jnp.where(key_down[:, :1] >= 0, per_slot * first + rank, -1.0)
    seats = lanes_for(slots * per_slot)
    for chunk in range(seats // 128):
        hot = jnp.broadcast_to(place, (items, 128)) == index_along((items, 128), 1) + 128 * chunk
        item = jnp.where(hot, index_along((items, 128), 0) - items, 0.0)
        chosen = items + jnp.sum(item, axis=0, keepdims=True)
        out[pl.ds(seat_row + chunk, 1), :] = chosen.astype(jnp.int32)
    for chunk in range(lanes // 128):
        out[pl.ds(last_row + chunk, 1), :] = last[:, 128 * chunk : 128 * (chunk + 1)].astype(
            jnp.int32
        )


def slots_for(items, groups):
    pairs = (items + min(items, groups)) // 2
    return -(-pairs // UNROLL) * UNROLL


def read_peers(peer_keys, lanes):
    items = peer_keys.shape[1]
    key_down = jnp.broadcast_to(peer_keys, (lanes_for(items), items)).T
    member = jnp.broadcast_to(key_down[:, :1], (items, lanes)) == index_along((items, lanes), 1)
    return jnp.sum(member.astype(jnp.float32), axis=0, keepdims=True)


def general(
    n,
    f_slots,
    b_slots,
    row_of,
    peer_of,
    live_count,
    rows_lane,
    peers_lane,
    need,
    source_hbm,
    target_hbm,
    tiles_hbm,
    source_out,
    target_out,
    x_out,
    x_ins,
    y_out,
    y_ins,
    x_now,
    y_now,
    y_base,
    f_sums,
    b_sums,
    c_sums,
    source,
    target,
    tiles,
    need_all,
    need_at,
    tile_plan,
    tile_at,
    part_plan,
    part_at,
    send_sem,
    recv_sem,
    need_send,
    need_recv,
    load_sem,
):
    me = lax.axis_index("rows")
    rows, side, width = source.shape
    tile_total = tiles_hbm.shape[0]
    f_seat, f_last = 0, lanes_for(2 * f_slots) // 128
    b_seat = f_last + lanes_for(rows) // 128
    b_last = b_seat + lanes_for(2 * b_slots) // 128
    c_last = lanes_for(n) // 128

    barrier = pltpu.get_barrier_semaphore()

    def greet(k, carry):
        pl.semaphore_signal(
            barrier, inc=1, device_id=(lax.rem(me + k, n),), device_id_type=MESH
        )
        return carry

    lax.fori_loop(1, n, greet, 0)
    source_load = pltpu.make_async_copy(source_hbm, source, load_sem.at[5])
    source_load.start()
    target_load = pltpu.make_async_copy(target_hbm, target, load_sem.at[0])
    target_load.start()
    tile_load = pltpu.make_async_copy(tiles_hbm, tiles.at[pl.ds(0, tile_total)], load_sem.at[1])
    tile_load.start()

    zero_block = jnp.zeros((side, width), jnp.bfloat16)
    zero_sum = jnp.zeros((side, width), jnp.float32)
    tiles[tile_total] = jnp.zeros((side, side), jnp.bfloat16)
    f_sums[f_slots] = zero_sum
    b_sums[b_slots] = zero_block
    c_sums[n] = zero_sum
    need_all[me] = need[...]
    pl.semaphore_wait(barrier, n - 1)

    def ask(k, carry):
        pltpu.make_async_remote_copy(
            src_ref=need,
            dst_ref=need_all.at[me],
            send_sem=need_send.at[0],
            recv_sem=need_recv.at[0],
            device_id=(lax.rem(me + k, n),),
            device_id_type=MESH,
        ).start()
        return carry

    lax.fori_loop(1, n, ask, 0)

    def turn(b, carry):
        flipped = target[b].astype(jnp.float32).T
        y_base[b] = flipped
        y_now[b] = flipped.astype(jnp.bfloat16)
        return carry

    def plan_tiles():
        live = lax.broadcasted_iota(jnp.int32, (1, tile_total), 1) < live_count[0]
        row_keys = jnp.where(live, rows_lane[...], -1).astype(jnp.float32)
        peer_keys = jnp.where(live, peers_lane[...], -1).astype(jnp.float32)
        place_groups(row_keys, rows, 2, f_slots, tile_plan, f_seat, f_last)
        place_groups(peer_keys, n, 2, b_slots, tile_plan, b_seat, b_last)
        load = pltpu.make_async_copy(tile_plan, tile_at, load_sem.at[3])
        load.start()
        load.wait()

    def plan_parts():
        table = need_all[...].reshape(n, need_all.shape[2]).astype(jnp.float32)
        mine = index_along(table.shape, 1) == me.astype(jnp.float32)
        wanted = jnp.sum(jnp.where(mine, table, 0.0), axis=1, keepdims=True)
        keys = jnp.broadcast_to(wanted, (n, 128)).T[:1]
        place_groups(keys, rows, 1, n, part_plan, 0, c_last)
        load = pltpu.make_async_copy(part_plan, part_at, load_sem.at[4])
        load.start()
        load.wait()

    def seat(table, first, index, top):
        return jnp.clip(table[first + index // 128, index % 128], 0, top)

    def tile_pair(first, q):
        left = seat(tile_at, first, 2 * q, tile_total)
        right = seat(tile_at, first, 2 * q + 1, tile_total)
        return left, right, jnp.minimum(left, tile_total - 1), jnp.minimum(right, tile_total - 1)

    def asked(d):
        return jnp.clip(need_at[d, 0, me], 0, rows - 1)

    def send(out, inn, phase, it, fill):
        def one(k, carry):
            peer = lax.rem(me + k, n)
            out[it, peer] = fill(peer)
            pltpu.make_async_remote_copy(
                src_ref=out.at[it, peer],
                dst_ref=inn.at[me],
                send_sem=send_sem.at[phase],
                recv_sem=recv_sem.at[phase],
                device_id=(peer,),
                device_id_type=MESH,
            ).start()
            return carry

        lax.fori_loop(1, n, one, 0)
        inn[me] = fill(me)

    def all_of(buffer, sem):
        view = buffer.at[pl.ds(0, n - 1)]
        pltpu.make_async_copy(view, view, sem).wait()

    def send_x(blocks, it):
        send(x_out, x_ins[it], 2 * it, it, lambda p: blocks[asked(p)])

    def backward(it):
        def one(q, carry):
            total, key = carry
            left, right, left_at, right_at = tile_pair(b_seat, q)
            flipped = jnp.concatenate([y_now[row_of[left_at]], y_now[row_of[right_at]]], axis=1)
            stack = jnp.concatenate([tiles[left], tiles[right]], axis=0)
            product = jnp.dot(flipped, stack, preferred_element_type=jnp.float32)
            new_key = peer_of[left_at]
            total = total * (new_key == key).astype(jnp.float32) + product
            b_sums[q] = total.astype(jnp.bfloat16)
            return total, new_key

        lax.fori_loop(0, b_slots, one, (zero_sum, jnp.int32(-1)), unroll=UNROLL)
        send(y_out, y_ins[it], 2 * it + 1, it, lambda p: b_sums[seat(tile_at, b_last, p, b_slots)])

    def forward(it, result):
        x_in = x_ins[it]
        all_of(x_in, recv_sem.at[2 * it])

        def one(q, carry):
            total, key = carry
            left, right, left_at, right_at = tile_pair(f_seat, q)
            stack = jnp.concatenate([tiles[left], tiles[right]], axis=1)
            blocks = jnp.concatenate([x_in[peer_of[left_at]], x_in[peer_of[right_at]]], axis=0)
            product = jnp.dot(stack, blocks, preferred_element_type=jnp.float32)
            new_key = row_of[left_at]
            total = total * (new_key == key).astype(jnp.float32) + product
            f_sums[q] = total
            return total, new_key

        lax.fori_loop(0, f_slots, one, (zero_sum, jnp.int32(-1)), unroll=UNROLL)

        def settle(b, carry):
            total = source[b].astype(jnp.float32) + f_sums[seat(tile_at, f_last, b, f_slots)]
            scale = lax.rsqrt(jnp.mean(total * total, axis=-1, keepdims=True) + epsilon)
            result[b] = (total * scale).astype(jnp.bfloat16)
            return carry

        lax.fori_loop(0, rows, settle, 0)

    def combine(it, final):
        y_in = y_ins[it]
        all_of(y_in, recv_sem.at[2 * it + 1])

        def one(k, carry):
            total, key = carry
            sender = seat(part_at, 0, k, n - 1)
            new_key = asked(sender)
            total = total * (new_key == key).astype(jnp.float32) + y_in[sender].astype(jnp.float32)
            c_sums[k] = total
            return total, new_key

        lax.fori_loop(0, n, one, (zero_sum, jnp.int32(-1)), unroll=UNROLL)

        def settle(b, carry):
            total = y_base[b] + c_sums[seat(part_at, c_last, b, n)]
            scale = lax.rsqrt(jnp.mean(total * total, axis=0, keepdims=True) + epsilon)
            if final:
                target_out[b] = (total * scale).T.astype(jnp.bfloat16)
            else:
                y_now[b] = (total * scale).astype(jnp.bfloat16)
            return carry

        lax.fori_loop(0, rows, settle, 0)

    all_of(need_all, need_recv.at[0])
    need_load = pltpu.make_async_copy(need_all, need_at, load_sem.at[2])
    need_load.start()
    need_load.wait()
    source_load.wait()
    send_x(source, 0)
    plan_tiles()
    target_load.wait()
    lax.fori_loop(0, rows, turn, 0)
    tile_load.wait()
    backward(0)
    plan_parts()
    for it in range(ITERS):
        final = it == ITERS - 1
        forward(it, source_out if final else x_now)
        if not final:
            send_x(x_now, it + 1)
        combine(it, final)
        if not final:
            backward(it + 1)
    all_of(need_all, need_send.at[0])
    for it in range(ITERS):
        all_of(x_out.at[it], send_sem.at[2 * it])
        all_of(y_out.at[it], send_sem.at[2 * it + 1])


def fast(
    n,
    cap,
    f_slots,
    b_slots,
    row_of,
    peer_of,
    live_count,
    rows_lane,
    peers_lane,
    need,
    source_hbm,
    target_hbm,
    tiles_hbm,
    source_out,
    target_out,
    over_out,
    x_near_out,
    x_far_out,
    x_ins,
    hubs,
    hub_out,
    gates,
    relay_out,
    y_out,
    y_near_ins,
    y_gates,
    y_cross_out,
    y_far_ins,
    x_now,
    y_now,
    y_base,
    y_mid,
    f_sums,
    b_sums,
    c_sums,
    source,
    target,
    tiles,
    need_mine,
    need_all,
    need_at,
    tile_plan,
    tile_at,
    part_plan,
    part_at,
    far_plan,
    far_at,
    x_send,
    x_recv,
    hub_send,
    hub_recv,
    spoke_send,
    gate_send,
    gate_recv,
    relay_send,
    y_send,
    y_near_recv,
    y_gate_recv,
    y_cross_send,
    y_far_recv,
    need_send,
    need_recv,
    load_sem,
):
    me = lax.axis_index("rows")
    rows, side, width = source.shape
    tile_total = tiles_hbm.shape[0]
    lanes = lanes_for(n)
    half, plane = n // 2, n // 4
    upper = me // half
    near_first, far_first = upper * half, (1 - upper) * half
    spot, column = me % half, me % plane
    inner = me // plane == 1 + upper
    outer = jnp.logical_not(inner)
    far_gate = (2 - upper) * plane + column
    near_gates = (1 + upper) * plane
    mine_first = me - column
    other_first = 2 * near_first + plane - mine_first
    near_gate = near_gates + column
    outer_owner = 3 * upper * plane + column
    far_planes = (3 * (1 - upper) * plane, (2 - upper) * plane)
    far_owner = tuple(first + column for first in far_planes)
    f_seat, f_last = 0, lanes_for(2 * f_slots) // 128
    b_seat = f_last + lanes_for(rows) // 128
    b_last = b_seat + lanes_for(2 * b_slots) // 128
    c_last = lanes_for(n) // 128
    part_rows = c_last + lanes_for(rows) // 128
    far_list = n
    far_slot = n + rows

    barrier = pltpu.get_barrier_semaphore()

    def greet(k, carry):
        pl.semaphore_signal(
            barrier, inc=1, device_id=(lax.rem(me + k, n),), device_id_type=MESH
        )
        return carry

    lax.fori_loop(1, n, greet, 0)
    source_load = pltpu.make_async_copy(source_hbm, source, load_sem.at[5])
    source_load.start()
    target_load = pltpu.make_async_copy(target_hbm, target, load_sem.at[0])
    target_load.start()
    tile_load = pltpu.make_async_copy(tiles_hbm, tiles.at[pl.ds(0, tile_total)], load_sem.at[1])
    tile_load.start()

    live = lax.broadcasted_iota(jnp.int32, (1, tile_total), 1) < live_count[0]
    row_keys = jnp.where(live, rows_lane[...], -1).astype(jnp.float32)
    peer_keys = jnp.where(live, peers_lane[...], -1).astype(jnp.float32)
    read = read_peers(peer_keys, lanes)
    need_mine[...] = jnp.full((1, lanes), -1, jnp.int32)
    need_mine[:, :n] = jnp.where(read[:, :n] > 0, need[...], -1)
    zero_block = jnp.zeros((side, width), jnp.bfloat16)
    zero_sum = jnp.zeros((side, width), jnp.float32)
    tiles[tile_total] = jnp.zeros((side, side), jnp.bfloat16)
    f_sums[f_slots] = zero_sum
    b_sums[b_slots] = zero_block
    c_sums[half] = zero_sum
    for it in range(ITERS):
        y_far_ins[it][cap] = zero_block
    need_all[me] = need_mine[...]
    def turn(b, carry):
        flipped = target[b].astype(jnp.float32).T
        y_base[b] = flipped
        y_now[b] = flipped.astype(jnp.bfloat16)
        return carry

    def plan_tiles():
        place_groups(row_keys, rows, 2, f_slots, tile_plan, f_seat, f_last)
        place_groups(peer_keys, n, 2, b_slots, tile_plan, b_seat, b_last)
        load = pltpu.make_async_copy(tile_plan, tile_at, load_sem.at[3])
        load.start()
        load.wait()

    plan_tiles()
    target_load.wait()
    lax.fori_loop(0, rows, turn, 0)
    source_load.wait()
    pl.semaphore_wait(barrier, n - 1)

    def push(src, dst, send_sem, recv_sem, peer):
        pltpu.make_async_remote_copy(
            src_ref=src,
            dst_ref=dst,
            send_sem=send_sem,
            recv_sem=recv_sem,
            device_id=(peer,),
            device_id_type=MESH,
        ).start()

    def all_of(buffer, count, sem):
        view = buffer.at[pl.ds(0, count)]
        pltpu.make_async_copy(view, view, sem).wait()

    def ask(k, carry):
        peer = lax.rem(me + k, n)
        push(need_mine, need_all.at[me], need_send.at[0], need_recv.at[0], peer)
        return carry

    lax.fori_loop(1, n, ask, 0)

    def needs():
        return need_all[...].reshape(n, lanes).astype(jnp.float32)

    def plan_far():
        table = needs()
        early = index_along((1, lanes), 1) < half
        before = jnp.zeros((1, lanes), jnp.float32)
        place = jnp.zeros((n, lanes), jnp.float32)
        listed = jnp.zeros((rows, lanes), jnp.float32)
        for b in range(rows):
            hit = (table == b).astype(jnp.float32)
            low = jnp.max(hit[:half], axis=0, keepdims=True)
            high = jnp.max(hit[half:], axis=0, keepdims=True)
            used = jnp.where(early, high, low)
            place = place + hit * before
            chosen = jnp.where(used > 0, before, -1.0)
            listed = jnp.where(index_along((rows, lanes), 0) == chosen, float(b), listed)
            far_plan[pl.ds(far_slot + b, 1), :] = jnp.where(used > 0, before, float(cap)).astype(
                jnp.int32
            )
            before = before + used
        far_plan[pl.ds(0, n), :] = place.astype(jnp.int32)
        far_plan[pl.ds(far_list, rows), :] = listed.astype(jnp.int32)
        worst = jnp.max(before, axis=1, keepdims=True)
        over_out[...] = (worst > cap).astype(jnp.int32)
        load = pltpu.make_async_copy(far_plan, far_at, load_sem.at[6])
        load.start()
        load.wait()

    def plan_parts():
        table = needs()
        sender = index_along((n, lanes), 0)
        lane = index_along((n, lanes), 1)
        near = (sender >= near_first.astype(jnp.float32)) & (
            sender < (near_first + half).astype(jnp.float32)
        )
        known = near & (table >= 0)
        place = far_plan[pl.ds(0, n), :].astype(jnp.float32)

        def column_of(values, at):
            mine = lane == at.astype(jnp.float32)
            column = jnp.sum(jnp.where(mine, values, 0.0), axis=1, keepdims=True)
            return jnp.broadcast_to(column, (n, 128)).T[:1]

        def plan(values, at, first):
            keys = column_of(jnp.where(known, values, -1.0), at)
            place_groups(keys, rows, 1, half, part_plan, first, first + c_last)

        plan(table, me, 0)
        for s in range(2):
            plan(place, far_owner[s], (1 + s) * part_rows)
        load = pltpu.make_async_copy(part_plan, part_at, load_sem.at[4])
        load.start()
        load.wait()

    def seat(table, first, index, top):
        return jnp.clip(table[first + index // 128, index % 128], 0, top)

    def tile_pair(first, q):
        left = seat(tile_at, first, 2 * q, tile_total)
        right = seat(tile_at, first, 2 * q + 1, tile_total)
        return left, right, jnp.minimum(left, tile_total - 1), jnp.minimum(right, tile_total - 1)

    def asked(d):
        return jnp.clip(need_at[d, 0, me], 0, rows - 1)

    def to_plane(one, first, low):
        def step(k, carry):
            one(first + lax.rem(column + k, plane), plane + k if low else k)
            return carry

        lax.fori_loop(low, plane, step, 0)

    def to_half(one, mine_ahead=False):
        legs = (other_first, 0), (mine_first, 1)
        for first, low in legs[::-1] if mine_ahead else legs:
            to_plane(one, first, low)

    def send_near(blocks, it):
        x_in = x_ins[it]

        def one(peer, k):
            x_near_out[k] = blocks[asked(peer)]
            push(x_near_out.at[k], x_in.at[me], x_send.at[it], x_recv.at[it], peer)

        if it:
            sent_near(it - 1)

        @pl.when(inner)
        def _():
            to_half(one)

        @pl.when(outer)
        def _():
            if it:
                to_plane(one, other_first, 0)
            to_plane(one, mine_first, 1)

        x_in[me] = blocks[asked(me)]

    def sent_near(it):
        @pl.when(inner)
        def _():
            all_of(x_near_out, half - 1, x_send.at[it])

        @pl.when(outer)
        def _():
            all_of(x_near_out, half - 1 if it else plane - 1, x_send.at[it])

    def pack_far(blocks, s, owner):
        def one(i, carry):
            x_far_out[s, i] = blocks[jnp.clip(far_at[far_list + i, owner], 0, rows - 1)]
            return carry

        lax.fori_loop(0, cap, one, 0)

    first_part = rows // 2
    hub_parts = (0, first_part, 0), (first_part, rows - first_part, ITERS)

    def send_hub_whole():
        for first, count, sem in hub_parts:
            piece = pl.ds(first, count)
            push(
                source.at[piece], hubs[0].at[piece], hub_send.at[0], hub_recv.at[sem], near_gate
            )

    def cross_hub_whole(half_at):
        first, count, sem = hub_parts[half_at]
        piece = pl.ds(first, count)
        all_of(hubs[0], count, hub_recv.at[sem])
        push(
            hubs[0].at[piece], gates[0][0].at[piece], gate_send.at[0], gate_recv.at[0], far_gate
        )

    def send_hub_packed():
        pack_far(x_now, 0, me)
        push(
            x_far_out.at[0],
            hubs[1].at[pl.ds(0, cap)],
            hub_send.at[1],
            hub_recv.at[1],
            near_gate,
        )

    def cross_hub_packed():
        all_of(hubs[1], cap, hub_recv.at[1])
        push(
            hubs[1].at[pl.ds(0, cap)],
            gates[1][0].at[pl.ds(0, cap)],
            gate_send.at[2],
            gate_recv.at[2],
            far_gate,
        )

    def send_far():
        pack_far(x_now, 1, me)
        push(
            x_far_out.at[1],
            gates[1][1].at[pl.ds(0, cap)],
            gate_send.at[3],
            gate_recv.at[3],
            far_gate,
        )

    def sent_far(it, s):
        all_of(gates[it][s], cap if it else rows, gate_send.at[2 * it + s])

    def serve_hub():
        held, x_in = hubs[0], x_ins[0]

        def block(d):
            return held[jnp.clip(need_at[d, 0, outer_owner], 0, rows - 1)]

        def one(k, carry):
            peer = near_gates + lax.rem(column + k, plane)
            hub_out[k] = block(peer)
            push(
                hub_out.at[k], x_in.at[outer_owner], spoke_send.at[0], x_recv.at[0], peer
            )
            return carry

        lax.fori_loop(1, plane, one, 0)
        x_in[outer_owner] = block(me)

    def relay(it, s, whole):
        gate, x_in, owner = gates[it][s], x_ins[it], far_owner[s]
        if it:
            all_of(x_in, half - 1, relay_send.at[2 * (it - 1) + s])
        all_of(gate, rows if whole else cap, gate_recv.at[2 * it + s])

        def block(d):
            at = need_at[d, 0, owner] if whole else far_at[d, owner]
            return gate[jnp.clip(at, 0, (rows if whole else cap) - 1)]

        def one(peer, k):
            relay_out[s, k] = block(peer)
            push(
                relay_out.at[s, k],
                x_in.at[owner],
                relay_send.at[2 * it + s],
                x_recv.at[it],
                peer,
            )

        to_half(one, it)
        x_in[owner] = block(me)

    def backward(it):
        def one(q, carry):
            total, key = carry
            left, right, left_at, right_at = tile_pair(b_seat, q)
            flipped = jnp.concatenate([y_now[row_of[left_at]], y_now[row_of[right_at]]], axis=1)
            stack = jnp.concatenate([tiles[left], tiles[right]], axis=0)
            product = jnp.dot(flipped, stack, preferred_element_type=jnp.float32)
            new_key = peer_of[left_at]
            total = total * (new_key == key).astype(jnp.float32) + product
            b_sums[q] = total.astype(jnp.bfloat16)
            return total, new_key

        lax.fori_loop(0, b_slots, one, (zero_sum, jnp.int32(-1)), unroll=UNROLL)

    def part(peer):
        return b_sums[seat(tile_at, b_last, peer, b_slots)]

    def send_parts(it, s):
        gate_in = y_gates[it][s]

        def one(k, carry):
            gate = lax.rem(column + k, plane)
            peer = far_planes[s] + gate
            y_out[peer] = part(peer)
            push(
                y_out.at[peer],
                gate_in.at[spot],
                y_send.at[it],
                y_gate_recv.at[2 * it + s],
                near_gates + gate,
            )
            return carry

        @pl.when(outer)
        def _():
            one(0, 0)

        @pl.when(inner)
        def _():
            gate_in[spot] = part(far_owner[s])

        lax.fori_loop(1, plane, one, 0)

    def send_near_parts(it):
        def one(peer, k):
            y_out[peer] = part(peer)
            push(y_out.at[peer], y_near_ins[it].at[spot], y_send.at[it], y_near_recv.at[it], peer)

        to_half(one)
        y_near_ins[it][spot] = part(me)

    def sent_parts(it):
        @pl.when(inner)
        def _():
            all_of(y_out, n - 3, y_send.at[it])

        @pl.when(outer)
        def _():
            all_of(y_out, n - 1, y_send.at[it])

    def forward(it, result):
        x_in = x_ins[it]

        @pl.when(inner)
        def _():
            all_of(x_in, n - 3 if it else n - 4, x_recv.at[it])

        @pl.when(outer)
        def _():
            all_of(x_in, n - 1, x_recv.at[it])

        def one(q, carry):
            total, key = carry
            left, right, left_at, right_at = tile_pair(f_seat, q)
            stack = jnp.concatenate([tiles[left], tiles[right]], axis=1)
            blocks = jnp.concatenate([x_in[peer_of[left_at]], x_in[peer_of[right_at]]], axis=0)
            product = jnp.dot(stack, blocks, preferred_element_type=jnp.float32)
            new_key = row_of[left_at]
            total = total * (new_key == key).astype(jnp.float32) + product
            f_sums[q] = total
            return total, new_key

        lax.fori_loop(0, f_slots, one, (zero_sum, jnp.int32(-1)), unroll=UNROLL)

        def settle(b, carry):
            total = source[b].astype(jnp.float32) + f_sums[seat(tile_at, f_last, b, f_slots)]
            scale = lax.rsqrt(jnp.mean(total * total, axis=-1, keepdims=True) + epsilon)
            result[b] = (total * scale).astype(jnp.bfloat16)
            return carry

        lax.fori_loop(0, rows, settle, 0)

    def gather(y_in, first, key_of):
        def one(k, carry):
            total, key = carry
            sender = seat(part_at, first, k, n - 1)
            new_key = key_of(sender)
            at = jnp.clip(sender - near_first, 0, half - 1)
            total = total * (new_key == key).astype(jnp.float32) + y_in[at].astype(jnp.float32)
            c_sums[k] = total
            return total, new_key

        lax.fori_loop(0, half, one, (zero_sum, jnp.int32(-1)), unroll=UNROLL)

    def cross_y(it, s):
        first = (1 + s) * part_rows
        all_of(y_gates[it][s], half - 1, y_gate_recv.at[2 * it + s])
        gather(y_gates[it][s], first, lambda d: far_at[d, far_owner[s]])
        if it:
            all_of(y_cross_out.at[s], cap, y_cross_send.at[2 * (it - 1) + s])

        def one(i, carry):
            total = c_sums[seat(part_at, first + c_last, i, half)]
            y_cross_out[s, i] = (total.T if it == ITERS - 1 else total).astype(jnp.bfloat16)
            return carry

        lax.fori_loop(0, cap, one, 0)
        push(
            y_cross_out.at[s],
            y_far_ins[it].at[pl.ds(0, cap)],
            y_cross_send.at[2 * it + s],
            y_far_recv.at[it],
            far_owner[s],
        )

    def combine_near(it):
        all_of(y_near_ins[it], half - 1, y_near_recv.at[it])
        gather(y_near_ins[it], 0, asked)

        def settle(b, carry):
            total = y_base[b] + c_sums[seat(part_at, c_last, b, half)]
            y_mid[b] = total.T if it == ITERS - 1 else total
            return carry

        lax.fori_loop(0, rows, settle, 0)

    def combine_far(it, final):
        y_far = y_far_ins[it]
        all_of(y_far, cap, y_far_recv.at[it])

        def settle(b, carry):
            at = jnp.clip(far_at[far_slot + b, me], 0, cap)
            total = y_mid[b] + y_far[at].astype(jnp.float32)
            over = -1 if final else 0
            scale = lax.rsqrt(jnp.mean(total * total, axis=over, keepdims=True) + epsilon)
            (target_out if final else y_now)[b] = (total * scale).astype(jnp.bfloat16)
            return carry

        lax.fori_loop(0, rows, settle, 0)

    def learn_needs():
        all_of(need_all, n - 1, need_recv.at[0])
        need_load = pltpu.make_async_copy(need_all, need_at, load_sem.at[2])
        need_load.start()
        plan_far()
        need_load.wait()

    @pl.when(inner)
    def _():
        push(source, gates[0][1], gate_send.at[1], gate_recv.at[1], far_gate)

    @pl.when(outer)
    def _():
        send_hub_whole()

    tile_load.wait()
    backward(0)
    send_parts(0, 1)
    send_parts(0, 0)
    learn_needs()
    send_near(source, 0)
    pl.when(inner)(functools.partial(cross_hub_whole, 0))
    pl.when(outer)(functools.partial(send_near_parts, 0))
    plan_parts()

    @pl.when(inner)
    def _():
        cross_hub_whole(1)
        serve_hub()
        relay(0, 1, True)
        send_near_parts(0)
        cross_y(0, 1)
        relay(0, 0, True)
        cross_y(0, 0)

    forward(0, x_now)

    @pl.when(inner)
    def _():
        send_far()

    @pl.when(outer)
    def _():
        send_hub_packed()

    pl.when(inner)(functools.partial(send_near, x_now, 1))
    combine_near(0)
    combine_far(0, False)
    backward(1)
    sent_parts(0)
    send_parts(1, 1)
    send_parts(1, 0)
    pl.when(outer)(functools.partial(send_near, x_now, 1))
    send_near_parts(1)

    @pl.when(inner)
    def _():
        relay(1, 1, False)
        cross_hub_packed()
        cross_y(1, 1)
        relay(1, 0, False)
        cross_y(1, 0)

    forward(1, source_out)
    combine_near(1)
    combine_far(1, True)

    all_of(need_all, n - 1, need_send.at[0])
    sent_near(ITERS - 1)
    sent_parts(ITERS - 1)

    @pl.when(outer)
    def _():
        for it in range(ITERS):
            all_of(hubs[it], cap if it else rows, hub_send.at[it])

    @pl.when(inner)
    def _():
        all_of(hub_out, plane - 1, spoke_send.at[0])
        for s in range(2):
            sent_far(0, s)
            sent_far(1, s)
            all_of(x_ins[0], half - 1, relay_send.at[2 * (ITERS - 1) + s])
            all_of(y_cross_out.at[s], cap, y_cross_send.at[2 * (ITERS - 1) + s])


def whole_exchange(source, target, tile_values, tile_rows, tile_peers, need_list, tile_count):
    n = lax.axis_size("rows")
    tiles_here, side, _ = tile_values.shape
    width = source.shape[1]
    rows = source.shape[0] // side
    f_slots = slots_for(tiles_here, rows)
    b_slots = slots_for(tiles_here, n)
    tile_plan = (
        lanes_for(2 * f_slots) + lanes_for(rows) + lanes_for(2 * b_slots) + lanes_for(n)
    ) // 128
    part_plan = (lanes_for(n) + lanes_for(rows)) // 128
    block = (side, width)
    vmem = pl.BlockSpec(memory_space=pltpu.VMEM)
    smem = pl.BlockSpec(memory_space=pltpu.SMEM)
    source_now, target_now = pl.pallas_call(
        functools.partial(general, n, f_slots, b_slots),
        out_shape=[pltpu.VMEM((rows,) + block, jnp.bfloat16)] * 2,
        in_specs=[smem] * 3 + [vmem] * 3 + [pl.BlockSpec(memory_space=pltpu.HBM)] * 3,
        out_specs=[vmem, vmem],
        scratch_shapes=[
            pltpu.VMEM((ITERS, n) + block, jnp.bfloat16),
            [pltpu.VMEM((n,) + block, jnp.bfloat16)] * ITERS,
            pltpu.VMEM((ITERS, n) + block, jnp.bfloat16),
            [pltpu.VMEM((n,) + block, jnp.bfloat16)] * ITERS,
            pltpu.VMEM((rows,) + block, jnp.bfloat16),
            pltpu.VMEM((rows,) + block, jnp.bfloat16),
            pltpu.VMEM((rows,) + block, jnp.float32),
            pltpu.VMEM((f_slots + 1,) + block, jnp.float32),
            pltpu.VMEM((b_slots + 1,) + block, jnp.bfloat16),
            pltpu.VMEM((n + 1,) + block, jnp.float32),
            pltpu.VMEM((rows,) + block, jnp.bfloat16),
            pltpu.VMEM((rows,) + block, jnp.bfloat16),
            pltpu.VMEM((tiles_here + 1, side, side), jnp.bfloat16),
            pltpu.VMEM((n, 1, n), jnp.int32),
            pltpu.SMEM((n, 1, n), jnp.int32),
            pltpu.VMEM((tile_plan, 128), jnp.int32),
            pltpu.SMEM((tile_plan, 128), jnp.int32),
            pltpu.VMEM((part_plan, 128), jnp.int32),
            pltpu.SMEM((part_plan, 128), jnp.int32),
            pltpu.SemaphoreType.DMA((2 * ITERS,)),
            pltpu.SemaphoreType.DMA((2 * ITERS,)),
            pltpu.SemaphoreType.DMA((1,)),
            pltpu.SemaphoreType.DMA((1,)),
            pltpu.SemaphoreType.DMA((6,)),
        ],
        compiler_params=pltpu.CompilerParams(
            collective_id=1, has_side_effects=True, vmem_limit_bytes=65000000
        ),
    )(
        tile_rows,
        tile_peers,
        tile_count,
        tile_rows.reshape(1, -1),
        tile_peers.reshape(1, -1),
        need_list,
        source.reshape((rows,) + block),
        target.reshape((rows,) + block),
        tile_values,
    )
    return source_now.reshape(-1, width), target_now.reshape(-1, width)


def shards(source, target, tile_values, tile_rows, tile_peers, need_list, tile_count):
    n = lax.axis_size("rows")
    tiles_here, side, _ = tile_values.shape
    width = source.shape[1]
    rows = source.shape[0] // side
    half, lanes = n // 2, lanes_for(n)
    cap = min(rows, 13)
    f_slots = slots_for(tiles_here, rows)
    b_slots = slots_for(tiles_here, n)
    tile_plan = (
        lanes_for(2 * f_slots) + lanes_for(rows) + lanes_for(2 * b_slots) + lanes_for(n)
    ) // 128
    part_plan = 3 * (lanes_for(n) + lanes_for(rows)) // 128
    far_plan = n + 2 * rows
    block = (side, width)
    vmem = pl.BlockSpec(memory_space=pltpu.VMEM)
    smem = pl.BlockSpec(memory_space=pltpu.SMEM)
    source_now, target_now, over = pl.pallas_call(
        functools.partial(fast, n, cap, f_slots, b_slots),
        out_shape=[pltpu.VMEM((rows,) + block, jnp.bfloat16)] * 2
        + [jax.ShapeDtypeStruct((1, 1), jnp.int32)],
        in_specs=[smem] * 3 + [vmem] * 3 + [pl.BlockSpec(memory_space=pltpu.HBM)] * 3,
        out_specs=[vmem] * 3,
        scratch_shapes=[
            pltpu.VMEM((half,) + block, jnp.bfloat16),
            pltpu.VMEM((2, cap) + block, jnp.bfloat16),
            [pltpu.VMEM((n,) + block, jnp.bfloat16)] * ITERS,
            [pltpu.VMEM((rows,) + block, jnp.bfloat16)] * ITERS,
            pltpu.VMEM((n // 4,) + block, jnp.bfloat16),
            [[pltpu.VMEM((rows,) + block, jnp.bfloat16)] * 2] * ITERS,
            pltpu.VMEM((2, half) + block, jnp.bfloat16),
            pltpu.VMEM((n,) + block, jnp.bfloat16),
            [pltpu.VMEM((half,) + block, jnp.bfloat16)] * ITERS,
            [[pltpu.VMEM((half,) + block, jnp.bfloat16)] * 2] * ITERS,
            pltpu.VMEM((2, cap) + block, jnp.bfloat16),
            [pltpu.VMEM((cap + 1,) + block, jnp.bfloat16)] * ITERS,
            pltpu.VMEM((rows,) + block, jnp.bfloat16),
            pltpu.VMEM((rows,) + block, jnp.bfloat16),
            pltpu.VMEM((rows,) + block, jnp.float32),
            pltpu.VMEM((rows,) + block, jnp.float32),
            pltpu.VMEM((f_slots + 1,) + block, jnp.float32),
            pltpu.VMEM((b_slots + 1,) + block, jnp.bfloat16),
            pltpu.VMEM((half + 1,) + block, jnp.float32),
            pltpu.VMEM((rows,) + block, jnp.bfloat16),
            pltpu.VMEM((rows,) + block, jnp.bfloat16),
            pltpu.VMEM((tiles_here + 1, side, side), jnp.bfloat16),
            pltpu.VMEM((1, lanes), jnp.int32),
            pltpu.VMEM((n, 1, lanes), jnp.int32),
            pltpu.SMEM((n, 1, lanes), jnp.int32),
            pltpu.VMEM((tile_plan, 128), jnp.int32),
            pltpu.SMEM((tile_plan, 128), jnp.int32),
            pltpu.VMEM((part_plan, 128), jnp.int32),
            pltpu.SMEM((part_plan, 128), jnp.int32),
            pltpu.VMEM((far_plan, lanes), jnp.int32),
            pltpu.SMEM((far_plan, lanes), jnp.int32),
            pltpu.SemaphoreType.DMA((ITERS,)),
            pltpu.SemaphoreType.DMA((ITERS,)),
            pltpu.SemaphoreType.DMA((ITERS,)),
            pltpu.SemaphoreType.DMA((ITERS + 1,)),
            pltpu.SemaphoreType.DMA((ITERS,)),
            pltpu.SemaphoreType.DMA((2 * ITERS,)),
            pltpu.SemaphoreType.DMA((2 * ITERS,)),
            pltpu.SemaphoreType.DMA((2 * ITERS,)),
            pltpu.SemaphoreType.DMA((ITERS,)),
            pltpu.SemaphoreType.DMA((ITERS,)),
            pltpu.SemaphoreType.DMA((2 * ITERS,)),
            pltpu.SemaphoreType.DMA((2 * ITERS,)),
            pltpu.SemaphoreType.DMA((ITERS,)),
            pltpu.SemaphoreType.DMA((1,)),
            pltpu.SemaphoreType.DMA((1,)),
            pltpu.SemaphoreType.DMA((7,)),
        ],
        compiler_params=pltpu.CompilerParams(
            collective_id=0, has_side_effects=True, vmem_limit_bytes=65000000
        ),
    )(
        tile_rows,
        tile_peers,
        tile_count,
        tile_rows.reshape(1, -1),
        tile_peers.reshape(1, -1),
        need_list,
        source.reshape((rows,) + block),
        target.reshape((rows,) + block),
        tile_values,
    )
    source_now, target_now = source_now.reshape(-1, width), target_now.reshape(-1, width)
    return lax.cond(
        over.reshape(()) > 0,
        lambda: whole_exchange(
            source, target, tile_values, tile_rows, tile_peers, need_list, tile_count
        ),
        lambda: (source_now, target_now),
    )


def solution(mesh):
    return jax.shard_map(
        shards,
        mesh=mesh,
        in_specs=(
            P("rows", None),
            P("rows", None),
            P("rows", None, None),
            P("rows"),
            P("rows"),
            P("rows", None),
            P("rows"),
        ),
        out_specs=(P("rows", None), P("rows", None)),
        check_vma=False,
    )
```

```python
import functools

import jax
import jax.numpy as jnp
from jax import lax
from jax.experimental import pallas as pl
from jax.experimental.pallas import tpu as pltpu
from jax.sharding import PartitionSpec as P

ITERS = 2
UNROLL = 4
epsilon = 1e-06
MESH = pl.DeviceIdType.MESH


def lanes_for(count):
    return -(-count // 128) * 128


def index_along(shape, axis):
    return lax.broadcasted_iota(jnp.int32, shape, axis).astype(jnp.float32)


def place_groups(keys, groups, per_slot, slots, out, seat_row, last_row):
    items, lanes = keys.shape[1], lanes_for(groups)
    key = jnp.broadcast_to(keys, (items, items))
    key_down = jnp.broadcast_to(keys, (lanes_for(items), items)).T
    before = (key_down[:, :items] == key) & (
        index_along((items, items), 1) < index_along((items, items), 0)
    )
    rank = jnp.sum(before.astype(jnp.float32), axis=1, keepdims=True)
    lane = index_along((items, lanes), 1)
    member = (jnp.broadcast_to(key_down[:, :1], (items, lanes)) == lane).astype(jnp.float32)
    count = jnp.sum(member, axis=0, keepdims=True)
    used = jnp.floor((count + (per_slot - 1)) * (1.0 / per_slot))
    used_down = jnp.broadcast_to(used, (lanes, lanes)).T
    earlier = (index_along((lanes, lanes), 0) < index_along((lanes, lanes), 1)).astype(jnp.float32)
    start = jnp.sum(used_down * earlier, axis=0, keepdims=True)
    last = jnp.where(used > 0, start + used - 1, float(slots))
    first = jnp.sum(member * start, axis=1, keepdims=True)
    place = jnp.where(key_down[:, :1] >= 0, per_slot * first + rank, -1.0)
    seats = lanes_for(slots * per_slot)
    for chunk in range(seats // 128):
        hot = jnp.broadcast_to(place, (items, 128)) == index_along((items, 128), 1) + 128 * chunk
        item = jnp.where(hot, index_along((items, 128), 0) - items, 0.0)
        chosen = items + jnp.sum(item, axis=0, keepdims=True)
        out[pl.ds(seat_row + chunk, 1), :] = chosen.astype(jnp.int32)
    for chunk in range(lanes // 128):
        out[pl.ds(last_row + chunk, 1), :] = last[:, 128 * chunk : 128 * (chunk + 1)].astype(
            jnp.int32
        )


def slots_for(items, groups):
    pairs = (items + min(items, groups)) // 2
    return -(-pairs // UNROLL) * UNROLL


def read_peers(peer_keys, lanes):
    items = peer_keys.shape[1]
    key_down = jnp.broadcast_to(peer_keys, (lanes_for(items), items)).T
    member = jnp.broadcast_to(key_down[:, :1], (items, lanes)) == index_along((items, lanes), 1)
    return jnp.sum(member.astype(jnp.float32), axis=0, keepdims=True)


def general(
    n,
    f_slots,
    b_slots,
    row_of,
    peer_of,
    live_count,
    rows_lane,
    peers_lane,
    need,
    source_hbm,
    target_hbm,
    tiles_hbm,
    source_out,
    target_out,
    x_out,
    x_ins,
    y_out,
    y_ins,
    x_now,
    y_now,
    y_base,
    f_sums,
    b_sums,
    c_sums,
    source,
    target,
    tiles,
    need_all,
    need_at,
    tile_plan,
    tile_at,
    part_plan,
    part_at,
    send_sem,
    recv_sem,
    need_send,
    need_recv,
    load_sem,
):
    me = lax.axis_index("rows")
    rows, side, width = source.shape
    tile_total = tiles_hbm.shape[0]
    f_seat, f_last = 0, lanes_for(2 * f_slots) // 128
    b_seat = f_last + lanes_for(rows) // 128
    b_last = b_seat + lanes_for(2 * b_slots) // 128
    c_last = lanes_for(n) // 128

    barrier = pltpu.get_barrier_semaphore()

    def greet(k, carry):
        pl.semaphore_signal(
            barrier, inc=1, device_id=(lax.rem(me + k, n),), device_id_type=MESH
        )
        return carry

    lax.fori_loop(1, n, greet, 0)
    source_load = pltpu.make_async_copy(source_hbm, source, load_sem.at[5])
    source_load.start()
    target_load = pltpu.make_async_copy(target_hbm, target, load_sem.at[0])
    target_load.start()
    tile_load = pltpu.make_async_copy(tiles_hbm, tiles.at[pl.ds(0, tile_total)], load_sem.at[1])
    tile_load.start()

    zero_block = jnp.zeros((side, width), jnp.bfloat16)
    zero_sum = jnp.zeros((side, width), jnp.float32)
    tiles[tile_total] = jnp.zeros((side, side), jnp.bfloat16)
    f_sums[f_slots] = zero_sum
    b_sums[b_slots] = zero_block
    c_sums[n] = zero_sum
    need_all[me] = need[...]
    pl.semaphore_wait(barrier, n - 1)

    def ask(k, carry):
        pltpu.make_async_remote_copy(
            src_ref=need,
            dst_ref=need_all.at[me],
            send_sem=need_send.at[0],
            recv_sem=need_recv.at[0],
            device_id=(lax.rem(me + k, n),),
            device_id_type=MESH,
        ).start()
        return carry

    lax.fori_loop(1, n, ask, 0)

    def turn(b, carry):
        flipped = target[b].astype(jnp.float32).T
        y_base[b] = flipped
        y_now[b] = flipped.astype(jnp.bfloat16)
        return carry

    def plan_tiles():
        live = lax.broadcasted_iota(jnp.int32, (1, tile_total), 1) < live_count[0]
        row_keys = jnp.where(live, rows_lane[...], -1).astype(jnp.float32)
        peer_keys = jnp.where(live, peers_lane[...], -1).astype(jnp.float32)
        place_groups(row_keys, rows, 2, f_slots, tile_plan, f_seat, f_last)
        place_groups(peer_keys, n, 2, b_slots, tile_plan, b_seat, b_last)
        load = pltpu.make_async_copy(tile_plan, tile_at, load_sem.at[3])
        load.start()
        load.wait()

    def plan_parts():
        table = need_all[...].reshape(n, need_all.shape[2]).astype(jnp.float32)
        mine = index_along(table.shape, 1) == me.astype(jnp.float32)
        wanted = jnp.sum(jnp.where(mine, table, 0.0), axis=1, keepdims=True)
        keys = jnp.broadcast_to(wanted, (n, 128)).T[:1]
        place_groups(keys, rows, 1, n, part_plan, 0, c_last)
        load = pltpu.make_async_copy(part_plan, part_at, load_sem.at[4])
        load.start()
        load.wait()

    def seat(table, first, index, top):
        return jnp.clip(table[first + index // 128, index % 128], 0, top)

    def tile_pair(first, q):
        left = seat(tile_at, first, 2 * q, tile_total)
        right = seat(tile_at, first, 2 * q + 1, tile_total)
        return left, right, jnp.minimum(left, tile_total - 1), jnp.minimum(right, tile_total - 1)

    def asked(d):
        return jnp.clip(need_at[d, 0, me], 0, rows - 1)

    def send(out, inn, phase, it, fill):
        def one(k, carry):
            peer = lax.rem(me + k, n)
            out[it, peer] = fill(peer)
            pltpu.make_async_remote_copy(
                src_ref=out.at[it, peer],
                dst_ref=inn.at[me],
                send_sem=send_sem.at[phase],
                recv_sem=recv_sem.at[phase],
                device_id=(peer,),
                device_id_type=MESH,
            ).start()
            return carry

        lax.fori_loop(1, n, one, 0)
        inn[me] = fill(me)

    def all_of(buffer, sem):
        view = buffer.at[pl.ds(0, n - 1)]
        pltpu.make_async_copy(view, view, sem).wait()

    def send_x(blocks, it):
        send(x_out, x_ins[it], 2 * it, it, lambda p: blocks[asked(p)])

    def backward(it):
        def one(q, carry):
            total, key = carry
            left, right, left_at, right_at = tile_pair(b_seat, q)
            flipped = jnp.concatenate([y_now[row_of[left_at]], y_now[row_of[right_at]]], axis=1)
            stack = jnp.concatenate([tiles[left], tiles[right]], axis=0)
            product = jnp.dot(flipped, stack, preferred_element_type=jnp.float32)
            new_key = peer_of[left_at]
            total = total * (new_key == key).astype(jnp.float32) + product
            b_sums[q] = total.astype(jnp.bfloat16)
            return total, new_key

        lax.fori_loop(0, b_slots, one, (zero_sum, jnp.int32(-1)), unroll=UNROLL)
        send(y_out, y_ins[it], 2 * it + 1, it, lambda p: b_sums[seat(tile_at, b_last, p, b_slots)])

    def forward(it, result):
        x_in = x_ins[it]
        all_of(x_in, recv_sem.at[2 * it])

        def one(q, carry):
            total, key = carry
            left, right, left_at, right_at = tile_pair(f_seat, q)
            stack = jnp.concatenate([tiles[left], tiles[right]], axis=1)
            blocks = jnp.concatenate([x_in[peer_of[left_at]], x_in[peer_of[right_at]]], axis=0)
            product = jnp.dot(stack, blocks, preferred_element_type=jnp.float32)
            new_key = row_of[left_at]
            total = total * (new_key == key).astype(jnp.float32) + product
            f_sums[q] = total
            return total, new_key

        lax.fori_loop(0, f_slots, one, (zero_sum, jnp.int32(-1)), unroll=UNROLL)

        def settle(b, carry):
            total = source[b].astype(jnp.float32) + f_sums[seat(tile_at, f_last, b, f_slots)]
            scale = lax.rsqrt(jnp.mean(total * total, axis=-1, keepdims=True) + epsilon)
            result[b] = (total * scale).astype(jnp.bfloat16)
            return carry

        lax.fori_loop(0, rows, settle, 0)

    def combine(it, final):
        y_in = y_ins[it]
        all_of(y_in, recv_sem.at[2 * it + 1])

        def one(k, carry):
            total, key = carry
            sender = seat(part_at, 0, k, n - 1)
            new_key = asked(sender)
            total = total * (new_key == key).astype(jnp.float32) + y_in[sender].astype(jnp.float32)
            c_sums[k] = total
            return total, new_key

        lax.fori_loop(0, n, one, (zero_sum, jnp.int32(-1)), unroll=UNROLL)

        def settle(b, carry):
            total = y_base[b] + c_sums[seat(part_at, c_last, b, n)]
            scale = lax.rsqrt(jnp.mean(total * total, axis=0, keepdims=True) + epsilon)
            if final:
                target_out[b] = (total * scale).T.astype(jnp.bfloat16)
            else:
                y_now[b] = (total * scale).astype(jnp.bfloat16)
            return carry

        lax.fori_loop(0, rows, settle, 0)

    all_of(need_all, need_recv.at[0])
    need_load = pltpu.make_async_copy(need_all, need_at, load_sem.at[2])
    need_load.start()
    need_load.wait()
    source_load.wait()
    send_x(source, 0)
    plan_tiles()
    target_load.wait()
    lax.fori_loop(0, rows, turn, 0)
    tile_load.wait()
    backward(0)
    plan_parts()
    for it in range(ITERS):
        final = it == ITERS - 1
        forward(it, source_out if final else x_now)
        if not final:
            send_x(x_now, it + 1)
        combine(it, final)
        if not final:
            backward(it + 1)
    all_of(need_all, need_send.at[0])
    for it in range(ITERS):
        all_of(x_out.at[it], send_sem.at[2 * it])
        all_of(y_out.at[it], send_sem.at[2 * it + 1])


def fast(
    n,
    cap,
    f_slots,
    b_slots,
    row_of,
    peer_of,
    live_count,
    rows_lane,
    peers_lane,
    need,
    source_hbm,
    target_hbm,
    tiles_hbm,
    source_out,
    target_out,
    over_out,
    x_near_out,
    x_far_out,
    x_ins,
    hubs,
    hub_out,
    gates,
    relay_out,
    y_out,
    y_near_ins,
    y_gates,
    y_cross_out,
    y_far_ins,
    x_now,
    y_now,
    y_base,
    y_mid,
    f_sums,
    b_sums,
    c_sums,
    source,
    target,
    tiles,
    need_mine,
    need_all,
    need_at,
    tile_plan,
    tile_at,
    part_plan,
    part_at,
    far_plan,
    far_at,
    over,
    x_send,
    x_recv,
    hub_send,
    hub_recv,
    spoke_send,
    gate_send,
    gate_recv,
    relay_send,
    y_send,
    y_near_recv,
    y_gate_recv,
    y_cross_send,
    y_far_recv,
    need_send,
    need_recv,
    load_sem,
):
    me = lax.axis_index("rows")
    rows, side, width = source.shape
    tile_total = tiles_hbm.shape[0]
    lanes = lanes_for(n)
    half, plane = n // 2, n // 4
    upper = me // half
    near_first, far_first = upper * half, (1 - upper) * half
    spot, column = me % half, me % plane
    inner = me // plane == 1 + upper
    outer = jnp.logical_not(inner)
    far_gate = (2 - upper) * plane + column
    near_gates = (1 + upper) * plane
    mine_first = me - column
    other_first = 2 * near_first + plane - mine_first
    near_gate = near_gates + column
    outer_owner = 3 * upper * plane + column
    far_planes = (3 * (1 - upper) * plane, (2 - upper) * plane)
    far_owner = tuple(first + column for first in far_planes)
    f_seat, f_last = 0, lanes_for(2 * f_slots) // 128
    b_seat = f_last + lanes_for(rows) // 128
    b_last = b_seat + lanes_for(2 * b_slots) // 128
    c_last = lanes_for(n) // 128
    part_rows = c_last + lanes_for(rows) // 128
    far_list = n
    far_slot = n + rows

    barrier = pltpu.get_barrier_semaphore()

    def greet(k, carry):
        pl.semaphore_signal(
            barrier, inc=1, device_id=(lax.rem(me + k, n),), device_id_type=MESH
        )
        return carry

    lax.fori_loop(1, n, greet, 0)
    source_load = pltpu.make_async_copy(source_hbm, source, load_sem.at[5])
    source_load.start()
    target_load = pltpu.make_async_copy(target_hbm, target, load_sem.at[0])
    target_load.start()
    tile_load = pltpu.make_async_copy(tiles_hbm, tiles.at[pl.ds(0, tile_total)], load_sem.at[1])
    tile_load.start()

    live = lax.broadcasted_iota(jnp.int32, (1, tile_total), 1) < live_count[0]
    row_keys = jnp.where(live, rows_lane[...], -1).astype(jnp.float32)
    peer_keys = jnp.where(live, peers_lane[...], -1).astype(jnp.float32)
    read = read_peers(peer_keys, lanes)
    need_mine[...] = jnp.full((1, lanes), -1, jnp.int32)
    need_mine[:, :n] = jnp.where(read[:, :n] > 0, need[...], -1)
    zero_block = jnp.zeros((side, width), jnp.bfloat16)
    zero_sum = jnp.zeros((side, width), jnp.float32)
    tiles[tile_total] = jnp.zeros((side, side), jnp.bfloat16)
    f_sums[f_slots] = zero_sum
    b_sums[b_slots] = zero_block
    c_sums[half] = zero_sum
    for it in range(ITERS):
        y_far_ins[it][cap] = zero_block
    need_all[me] = need_mine[...]
    def turn(b, carry):
        flipped = target[b].astype(jnp.float32).T
        y_base[b] = flipped
        y_now[b] = flipped.astype(jnp.bfloat16)
        return carry

    def plan_tiles():
        place_groups(row_keys, rows, 2, f_slots, tile_plan, f_seat, f_last)
        place_groups(peer_keys, n, 2, b_slots, tile_plan, b_seat, b_last)
        load = pltpu.make_async_copy(tile_plan, tile_at, load_sem.at[3])
        load.start()
        load.wait()

    plan_tiles()
    target_load.wait()
    lax.fori_loop(0, rows, turn, 0)
    source_load.wait()
    pl.semaphore_wait(barrier, n - 1)

    def push(src, dst, send_sem, recv_sem, peer):
        pltpu.make_async_remote_copy(
            src_ref=src,
            dst_ref=dst,
            send_sem=send_sem,
            recv_sem=recv_sem,
            device_id=(peer,),
            device_id_type=MESH,
        ).start()

    def all_of(buffer, count, sem):
        view = buffer.at[pl.ds(0, count)]
        pltpu.make_async_copy(view, view, sem).wait()

    def ask(k, carry):
        peer = lax.rem(me + k, n)
        push(need_mine, need_all.at[me], need_send.at[0], need_recv.at[0], peer)
        return carry

    lax.fori_loop(1, n, ask, 0)

    def needs():
        return need_all[...].reshape(n, lanes).astype(jnp.float32)

    def plan_far():
        table = needs()
        early = index_along((1, lanes), 1) < half
        before = jnp.zeros((1, lanes), jnp.float32)
        place = jnp.zeros((n, lanes), jnp.float32)
        listed = jnp.zeros((rows, lanes), jnp.float32)
        for b in range(rows):
            hit = (table == b).astype(jnp.float32)
            low = jnp.max(hit[:half], axis=0, keepdims=True)
            high = jnp.max(hit[half:], axis=0, keepdims=True)
            used = jnp.where(early, high, low)
            place = place + hit * before
            chosen = jnp.where(used > 0, before, -1.0)
            listed = jnp.where(index_along((rows, lanes), 0) == chosen, float(b), listed)
            far_plan[pl.ds(far_slot + b, 1), :] = jnp.where(used > 0, before, float(cap)).astype(
                jnp.int32
            )
            before = before + used
        far_plan[pl.ds(0, n), :] = place.astype(jnp.int32)
        far_plan[pl.ds(far_list, rows), :] = listed.astype(jnp.int32)
        worst = jnp.max(before, axis=1, keepdims=True)
        over[...] = (worst > cap).astype(jnp.int32)
        pltpu.make_async_copy(over, over_out, load_sem.at[7]).start()
        load = pltpu.make_async_copy(far_plan, far_at, load_sem.at[6])
        load.start()
        load.wait()

    def plan_parts():
        table = needs()
        sender = index_along((n, lanes), 0)
        lane = index_along((n, lanes), 1)
        near = (sender >= near_first.astype(jnp.float32)) & (
            sender < (near_first + half).astype(jnp.float32)
        )
        known = near & (table >= 0)
        place = far_plan[pl.ds(0, n), :].astype(jnp.float32)

        def column_of(values, at):
            mine = lane == at.astype(jnp.float32)
            column = jnp.sum(jnp.where(mine, values, 0.0), axis=1, keepdims=True)
            return jnp.broadcast_to(column, (n, 128)).T[:1]

        def plan(values, at, first):
            keys = column_of(jnp.where(known, values, -1.0), at)
            place_groups(keys, rows, 1, half, part_plan, first, first + c_last)

        plan(table, me, 0)
        for s in range(2):
            plan(place, far_owner[s], (1 + s) * part_rows)
        load = pltpu.make_async_copy(part_plan, part_at, load_sem.at[4])
        load.start()
        load.wait()

    def seat(table, first, index, top):
        return jnp.clip(table[first + index // 128, index % 128], 0, top)

    def tile_pair(first, q):
        left = seat(tile_at, first, 2 * q, tile_total)
        right = seat(tile_at, first, 2 * q + 1, tile_total)
        return left, right, jnp.minimum(left, tile_total - 1), jnp.minimum(right, tile_total - 1)

    def asked(d):
        return jnp.clip(need_at[d, 0, me], 0, rows - 1)

    def to_plane(one, first, low):
        def step(k, carry):
            one(first + lax.rem(column + k, plane), plane + k if low else k)
            return carry

        lax.fori_loop(low, plane, step, 0)

    def to_half(one, mine_ahead=False):
        legs = (other_first, 0), (mine_first, 1)
        for first, low in legs[::-1] if mine_ahead else legs:
            to_plane(one, first, low)

    def send_near(blocks, it):
        x_in = x_ins[it]

        def one(peer, k):
            x_near_out[k] = blocks[asked(peer)]
            push(x_near_out.at[k], x_in.at[me], x_send.at[it], x_recv.at[it], peer)

        if it:
            sent_near(it - 1)

        @pl.when(inner)
        def _():
            to_half(one)

        @pl.when(outer)
        def _():
            if it:
                to_plane(one, other_first, 0)
            to_plane(one, mine_first, 1)

        x_in[me] = blocks[asked(me)]

    def sent_near(it):
        @pl.when(inner)
        def _():
            all_of(x_near_out, half - 1, x_send.at[it])

        @pl.when(outer)
        def _():
            all_of(x_near_out, half - 1 if it else plane - 1, x_send.at[it])

    def pack_far(blocks, s, owner):
        def one(i, carry):
            x_far_out[s, i] = blocks[jnp.clip(far_at[far_list + i, owner], 0, rows - 1)]
            return carry

        lax.fori_loop(0, cap, one, 0)

    first_part = rows // 2
    hub_parts = (0, first_part, 0), (first_part, rows - first_part, ITERS)

    def send_hub_whole():
        for first, count, sem in hub_parts:
            piece = pl.ds(first, count)
            push(
                source.at[piece], hubs[0].at[piece], hub_send.at[0], hub_recv.at[sem], near_gate
            )

    def cross_hub_whole(half_at):
        first, count, sem = hub_parts[half_at]
        piece = pl.ds(first, count)
        all_of(hubs[0], count, hub_recv.at[sem])
        push(
            hubs[0].at[piece], gates[0][0].at[piece], gate_send.at[0], gate_recv.at[0], far_gate
        )

    def send_hub_packed():
        pack_far(x_now, 0, me)
        push(
            x_far_out.at[0],
            hubs[1].at[pl.ds(0, cap)],
            hub_send.at[1],
            hub_recv.at[1],
            near_gate,
        )

    def cross_hub_packed():
        all_of(hubs[1], cap, hub_recv.at[1])
        push(
            hubs[1].at[pl.ds(0, cap)],
            gates[1][0].at[pl.ds(0, cap)],
            gate_send.at[2],
            gate_recv.at[2],
            far_gate,
        )

    def send_far():
        pack_far(x_now, 1, me)
        push(
            x_far_out.at[1],
            gates[1][1].at[pl.ds(0, cap)],
            gate_send.at[3],
            gate_recv.at[3],
            far_gate,
        )

    def sent_far(it, s):
        all_of(gates[it][s], cap if it else rows, gate_send.at[2 * it + s])

    def serve_hub():
        held, x_in = hubs[0], x_ins[0]

        def block(d):
            return held[jnp.clip(need_at[d, 0, outer_owner], 0, rows - 1)]

        def one(k, carry):
            peer = near_gates + lax.rem(column + k, plane)
            hub_out[k] = block(peer)
            push(
                hub_out.at[k], x_in.at[outer_owner], spoke_send.at[0], x_recv.at[0], peer
            )
            return carry

        lax.fori_loop(1, plane, one, 0)
        x_in[outer_owner] = block(me)

    def relay(it, s, whole):
        gate, x_in, owner = gates[it][s], x_ins[it], far_owner[s]
        if it:
            all_of(x_in, half - 1, relay_send.at[2 * (it - 1) + s])
        all_of(gate, rows if whole else cap, gate_recv.at[2 * it + s])

        def block(d):
            at = need_at[d, 0, owner] if whole else far_at[d, owner]
            return gate[jnp.clip(at, 0, (rows if whole else cap) - 1)]

        def one(peer, k):
            relay_out[s, k] = block(peer)
            push(
                relay_out.at[s, k],
                x_in.at[owner],
                relay_send.at[2 * it + s],
                x_recv.at[it],
                peer,
            )

        to_half(one, it)
        x_in[owner] = block(me)

    def backward(it):
        def one(q, carry):
            total, key = carry
            left, right, left_at, right_at = tile_pair(b_seat, q)
            flipped = jnp.concatenate([y_now[row_of[left_at]], y_now[row_of[right_at]]], axis=1)
            stack = jnp.concatenate([tiles[left], tiles[right]], axis=0)
            product = jnp.dot(flipped, stack, preferred_element_type=jnp.float32)
            new_key = peer_of[left_at]
            total = total * (new_key == key).astype(jnp.float32) + product
            b_sums[q] = total.astype(jnp.bfloat16)
            return total, new_key

        lax.fori_loop(0, b_slots, one, (zero_sum, jnp.int32(-1)), unroll=UNROLL)

    def part(peer):
        return b_sums[seat(tile_at, b_last, peer, b_slots)]

    def send_parts(it, s):
        gate_in = y_gates[it][s]

        def one(k, carry):
            gate = lax.rem(column + k, plane)
            peer = far_planes[s] + gate
            y_out[peer] = part(peer)
            push(
                y_out.at[peer],
                gate_in.at[spot],
                y_send.at[it],
                y_gate_recv.at[2 * it + s],
                near_gates + gate,
            )
            return carry

        @pl.when(outer)
        def _():
            one(0, 0)

        @pl.when(inner)
        def _():
            gate_in[spot] = part(far_owner[s])

        lax.fori_loop(1, plane, one, 0)

    def send_near_parts(it):
        def one(peer, k):
            y_out[peer] = part(peer)
            push(y_out.at[peer], y_near_ins[it].at[spot], y_send.at[it], y_near_recv.at[it], peer)

        to_half(one)
        y_near_ins[it][spot] = part(me)

    def sent_parts(it):
        @pl.when(inner)
        def _():
            all_of(y_out, n - 3, y_send.at[it])

        @pl.when(outer)
        def _():
            all_of(y_out, n - 1, y_send.at[it])

    def forward(it, result):
        x_in = x_ins[it]

        @pl.when(inner)
        def _():
            all_of(x_in, n - 3 if it else n - 4, x_recv.at[it])

        @pl.when(outer)
        def _():
            all_of(x_in, n - 1, x_recv.at[it])

        def one(q, carry):
            total, key = carry
            left, right, left_at, right_at = tile_pair(f_seat, q)
            stack = jnp.concatenate([tiles[left], tiles[right]], axis=1)
            blocks = jnp.concatenate([x_in[peer_of[left_at]], x_in[peer_of[right_at]]], axis=0)
            product = jnp.dot(stack, blocks, preferred_element_type=jnp.float32)
            new_key = row_of[left_at]
            total = total * (new_key == key).astype(jnp.float32) + product
            f_sums[q] = total
            return total, new_key

        lax.fori_loop(0, f_slots, one, (zero_sum, jnp.int32(-1)), unroll=UNROLL)

        def settle(b, carry):
            total = source[b].astype(jnp.float32) + f_sums[seat(tile_at, f_last, b, f_slots)]
            scale = lax.rsqrt(jnp.mean(total * total, axis=-1, keepdims=True) + epsilon)
            result[b] = (total * scale).astype(jnp.bfloat16)
            return carry

        lax.fori_loop(0, rows, settle, 0)

    def gather(y_in, first, key_of):
        def one(k, carry):
            total, key = carry
            sender = seat(part_at, first, k, n - 1)
            new_key = key_of(sender)
            at = jnp.clip(sender - near_first, 0, half - 1)
            total = total * (new_key == key).astype(jnp.float32) + y_in[at].astype(jnp.float32)
            c_sums[k] = total
            return total, new_key

        lax.fori_loop(0, half, one, (zero_sum, jnp.int32(-1)), unroll=UNROLL)

    def cross_y(it, s):
        first = (1 + s) * part_rows
        all_of(y_gates[it][s], half - 1, y_gate_recv.at[2 * it + s])
        gather(y_gates[it][s], first, lambda d: far_at[d, far_owner[s]])
        if it:
            all_of(y_cross_out.at[s], cap, y_cross_send.at[2 * (it - 1) + s])

        def one(i, carry):
            total = c_sums[seat(part_at, first + c_last, i, half)]
            y_cross_out[s, i] = (total.T if it == ITERS - 1 else total).astype(jnp.bfloat16)
            return carry

        lax.fori_loop(0, cap, one, 0)
        push(
            y_cross_out.at[s],
            y_far_ins[it].at[pl.ds(0, cap)],
            y_cross_send.at[2 * it + s],
            y_far_recv.at[it],
            far_owner[s],
        )

    def combine_near(it):
        all_of(y_near_ins[it], half - 1, y_near_recv.at[it])
        gather(y_near_ins[it], 0, asked)

        def settle(b, carry):
            total = y_base[b] + c_sums[seat(part_at, c_last, b, half)]
            y_mid[b] = total.T if it == ITERS - 1 else total
            return carry

        lax.fori_loop(0, rows, settle, 0)

    def combine_far(it, final):
        y_far = y_far_ins[it]
        all_of(y_far, cap, y_far_recv.at[it])

        def settle(b, carry):
            at = jnp.clip(far_at[far_slot + b, me], 0, cap)
            total = y_mid[b] + y_far[at].astype(jnp.float32)
            over = -1 if final else 0
            scale = lax.rsqrt(jnp.mean(total * total, axis=over, keepdims=True) + epsilon)
            (target_out if final else y_now)[b] = (total * scale).astype(jnp.bfloat16)
            return carry

        lax.fori_loop(0, rows, settle, 0)

    def learn_needs():
        all_of(need_all, n - 1, need_recv.at[0])
        need_load = pltpu.make_async_copy(need_all, need_at, load_sem.at[2])
        need_load.start()
        plan_far()
        need_load.wait()

    @pl.when(inner)
    def _():
        push(source, gates[0][1], gate_send.at[1], gate_recv.at[1], far_gate)

    @pl.when(outer)
    def _():
        send_hub_whole()

    tile_load.wait()
    backward(0)
    send_parts(0, 1)
    send_parts(0, 0)
    learn_needs()
    send_near(source, 0)
    pl.when(inner)(functools.partial(cross_hub_whole, 0))
    pl.when(outer)(functools.partial(send_near_parts, 0))
    plan_parts()

    @pl.when(inner)
    def _():
        cross_hub_whole(1)
        serve_hub()
        relay(0, 1, True)
        send_near_parts(0)
        cross_y(0, 1)
        relay(0, 0, True)
        cross_y(0, 0)

    forward(0, x_now)

    @pl.when(inner)
    def _():
        send_far()

    @pl.when(outer)
    def _():
        send_hub_packed()

    pl.when(inner)(functools.partial(send_near, x_now, 1))
    combine_near(0)
    combine_far(0, False)
    backward(1)
    sent_parts(0)
    send_parts(1, 1)
    send_parts(1, 0)
    pl.when(outer)(functools.partial(send_near, x_now, 1))
    send_near_parts(1)

    @pl.when(inner)
    def _():
        relay(1, 1, False)
        cross_hub_packed()
        cross_y(1, 1)
        relay(1, 0, False)
        cross_y(1, 0)

    forward(1, source_out)
    combine_near(1)
    combine_far(1, True)

    all_of(need_all, n - 1, need_send.at[0])
    pltpu.make_async_copy(over, over_out, load_sem.at[7]).wait()
    sent_near(ITERS - 1)
    sent_parts(ITERS - 1)

    @pl.when(outer)
    def _():
        for it in range(ITERS):
            all_of(hubs[it], cap if it else rows, hub_send.at[it])

    @pl.when(inner)
    def _():
        all_of(hub_out, plane - 1, spoke_send.at[0])
        for s in range(2):
            sent_far(0, s)
            sent_far(1, s)
            all_of(x_ins[0], half - 1, relay_send.at[2 * (ITERS - 1) + s])
            all_of(y_cross_out.at[s], cap, y_cross_send.at[2 * (ITERS - 1) + s])


def whole_exchange(source, target, tile_values, tile_rows, tile_peers, need_list, tile_count):
    n = lax.axis_size("rows")
    tiles_here, side, _ = tile_values.shape
    width = source.shape[1]
    rows = source.shape[0] // side
    f_slots = slots_for(tiles_here, rows)
    b_slots = slots_for(tiles_here, n)
    tile_plan = (
        lanes_for(2 * f_slots) + lanes_for(rows) + lanes_for(2 * b_slots) + lanes_for(n)
    ) // 128
    part_plan = (lanes_for(n) + lanes_for(rows)) // 128
    block = (side, width)
    vmem = pl.BlockSpec(memory_space=pltpu.VMEM)
    smem = pl.BlockSpec(memory_space=pltpu.SMEM)
    source_now, target_now = pl.pallas_call(
        functools.partial(general, n, f_slots, b_slots),
        out_shape=[pltpu.VMEM((rows,) + block, jnp.bfloat16)] * 2,
        in_specs=[smem] * 3 + [vmem] * 3 + [pl.BlockSpec(memory_space=pltpu.HBM)] * 3,
        out_specs=[vmem, vmem],
        scratch_shapes=[
            pltpu.VMEM((ITERS, n) + block, jnp.bfloat16),
            [pltpu.VMEM((n,) + block, jnp.bfloat16)] * ITERS,
            pltpu.VMEM((ITERS, n) + block, jnp.bfloat16),
            [pltpu.VMEM((n,) + block, jnp.bfloat16)] * ITERS,
            pltpu.VMEM((rows,) + block, jnp.bfloat16),
            pltpu.VMEM((rows,) + block, jnp.bfloat16),
            pltpu.VMEM((rows,) + block, jnp.float32),
            pltpu.VMEM((f_slots + 1,) + block, jnp.float32),
            pltpu.VMEM((b_slots + 1,) + block, jnp.bfloat16),
            pltpu.VMEM((n + 1,) + block, jnp.float32),
            pltpu.VMEM((rows,) + block, jnp.bfloat16),
            pltpu.VMEM((rows,) + block, jnp.bfloat16),
            pltpu.VMEM((tiles_here + 1, side, side), jnp.bfloat16),
            pltpu.VMEM((n, 1, n), jnp.int32),
            pltpu.SMEM((n, 1, n), jnp.int32),
            pltpu.VMEM((tile_plan, 128), jnp.int32),
            pltpu.SMEM((tile_plan, 128), jnp.int32),
            pltpu.VMEM((part_plan, 128), jnp.int32),
            pltpu.SMEM((part_plan, 128), jnp.int32),
            pltpu.SemaphoreType.DMA((2 * ITERS,)),
            pltpu.SemaphoreType.DMA((2 * ITERS,)),
            pltpu.SemaphoreType.DMA((1,)),
            pltpu.SemaphoreType.DMA((1,)),
            pltpu.SemaphoreType.DMA((6,)),
        ],
        compiler_params=pltpu.CompilerParams(
            collective_id=1, has_side_effects=True, vmem_limit_bytes=65000000
        ),
    )(
        tile_rows,
        tile_peers,
        tile_count,
        tile_rows.reshape(1, -1),
        tile_peers.reshape(1, -1),
        need_list,
        source.reshape((rows,) + block),
        target.reshape((rows,) + block),
        tile_values,
    )
    return source_now.reshape(-1, width), target_now.reshape(-1, width)


def shards(source, target, tile_values, tile_rows, tile_peers, need_list, tile_count):
    n = lax.axis_size("rows")
    tiles_here, side, _ = tile_values.shape
    width = source.shape[1]
    rows = source.shape[0] // side
    half, lanes = n // 2, lanes_for(n)
    cap = min(rows, 13)
    f_slots = slots_for(tiles_here, rows)
    b_slots = slots_for(tiles_here, n)
    tile_plan = (
        lanes_for(2 * f_slots) + lanes_for(rows) + lanes_for(2 * b_slots) + lanes_for(n)
    ) // 128
    part_plan = 3 * (lanes_for(n) + lanes_for(rows)) // 128
    far_plan = n + 2 * rows
    block = (side, width)
    vmem = pl.BlockSpec(memory_space=pltpu.VMEM)
    smem = pl.BlockSpec(memory_space=pltpu.SMEM)
    source_now, target_now, over = pl.pallas_call(
        functools.partial(fast, n, cap, f_slots, b_slots),
        out_shape=[pltpu.VMEM((rows,) + block, jnp.bfloat16)] * 2
        + [jax.ShapeDtypeStruct((1, 1), jnp.int32)],
        in_specs=[smem] * 3 + [vmem] * 3 + [pl.BlockSpec(memory_space=pltpu.HBM)] * 3,
        out_specs=[vmem] * 2 + [pl.BlockSpec(memory_space=pltpu.HBM)],
        scratch_shapes=[
            pltpu.VMEM((half,) + block, jnp.bfloat16),
            pltpu.VMEM((2, cap) + block, jnp.bfloat16),
            [pltpu.VMEM((n,) + block, jnp.bfloat16)] * ITERS,
            [pltpu.VMEM((rows,) + block, jnp.bfloat16)] * ITERS,
            pltpu.VMEM((n // 4,) + block, jnp.bfloat16),
            [[pltpu.VMEM((rows,) + block, jnp.bfloat16)] * 2] * ITERS,
            pltpu.VMEM((2, half) + block, jnp.bfloat16),
            pltpu.VMEM((n,) + block, jnp.bfloat16),
            [pltpu.VMEM((half,) + block, jnp.bfloat16)] * ITERS,
            [[pltpu.VMEM((half,) + block, jnp.bfloat16)] * 2] * ITERS,
            pltpu.VMEM((2, cap) + block, jnp.bfloat16),
            [pltpu.VMEM((cap + 1,) + block, jnp.bfloat16)] * ITERS,
            pltpu.VMEM((rows,) + block, jnp.bfloat16),
            pltpu.VMEM((rows,) + block, jnp.bfloat16),
            pltpu.VMEM((rows,) + block, jnp.float32),
            pltpu.VMEM((rows,) + block, jnp.float32),
            pltpu.VMEM((f_slots + 1,) + block, jnp.float32),
            pltpu.VMEM((b_slots + 1,) + block, jnp.bfloat16),
            pltpu.VMEM((half + 1,) + block, jnp.float32),
            pltpu.VMEM((rows,) + block, jnp.bfloat16),
            pltpu.VMEM((rows,) + block, jnp.bfloat16),
            pltpu.VMEM((tiles_here + 1, side, side), jnp.bfloat16),
            pltpu.VMEM((1, lanes), jnp.int32),
            pltpu.VMEM((n, 1, lanes), jnp.int32),
            pltpu.SMEM((n, 1, lanes), jnp.int32),
            pltpu.VMEM((tile_plan, 128), jnp.int32),
            pltpu.SMEM((tile_plan, 128), jnp.int32),
            pltpu.VMEM((part_plan, 128), jnp.int32),
            pltpu.SMEM((part_plan, 128), jnp.int32),
            pltpu.VMEM((far_plan, lanes), jnp.int32),
            pltpu.SMEM((far_plan, lanes), jnp.int32),
            pltpu.VMEM((1, 1), jnp.int32),
            pltpu.SemaphoreType.DMA((ITERS,)),
            pltpu.SemaphoreType.DMA((ITERS,)),
            pltpu.SemaphoreType.DMA((ITERS,)),
            pltpu.SemaphoreType.DMA((ITERS + 1,)),
            pltpu.SemaphoreType.DMA((ITERS,)),
            pltpu.SemaphoreType.DMA((2 * ITERS,)),
            pltpu.SemaphoreType.DMA((2 * ITERS,)),
            pltpu.SemaphoreType.DMA((2 * ITERS,)),
            pltpu.SemaphoreType.DMA((ITERS,)),
            pltpu.SemaphoreType.DMA((ITERS,)),
            pltpu.SemaphoreType.DMA((2 * ITERS,)),
            pltpu.SemaphoreType.DMA((2 * ITERS,)),
            pltpu.SemaphoreType.DMA((ITERS,)),
            pltpu.SemaphoreType.DMA((1,)),
            pltpu.SemaphoreType.DMA((1,)),
            pltpu.SemaphoreType.DMA((8,)),
        ],
        compiler_params=pltpu.CompilerParams(
            collective_id=0, has_side_effects=True, vmem_limit_bytes=65000000
        ),
    )(
        tile_rows,
        tile_peers,
        tile_count,
        tile_rows.reshape(1, -1),
        tile_peers.reshape(1, -1),
        need_list,
        source.reshape((rows,) + block),
        target.reshape((rows,) + block),
        tile_values,
    )
    source_now, target_now = source_now.reshape(-1, width), target_now.reshape(-1, width)
    return lax.cond(
        over.reshape(()) > 0,
        lambda: whole_exchange(
            source, target, tile_values, tile_rows, tile_peers, need_list, tile_count
        ),
        lambda: (source_now, target_now),
    )


def solution(mesh):
    return jax.shard_map(
        shards,
        mesh=mesh,
        in_specs=(
            P("rows", None),
            P("rows", None),
            P("rows", None, None),
            P("rows"),
            P("rows"),
            P("rows", None),
            P("rows"),
        ),
        out_specs=(P("rows", None), P("rows", None)),
        check_vma=False,
    )
```
